8 devices in a mesh: data: 1 (over z), dap: 8 (over y, x, core).
Axes of the slice: x: 2, y: 2, z: 1, core: 2. Of those that a mesh axis runs over, the one named last changes fastest.
Arguments:
- extra_msa: bfloat16 [3072, 256, 64], P('data', 'dap')
- extra_mask: int32 [3072, 256], P('data')
- main_msa: bfloat16 [512, 256, 256], P('data', 'dap')
- main_mask: int32 [512, 256], P('data')
- pair_act: float32 [256, 256, 128], P(('data', 'dap'))
- extra_ln_gamma: bfloat16 [64], replicated
- extra_ln_beta: bfloat16 [64], replicated
- extra_w_left: bfloat16 [64, 32], replicated
- extra_b_left: bfloat16 [32], replicated
- extra_w_right: bfloat16 [64, 32], replicated
- extra_b_right: bfloat16 [32], replicated
- extra_w_out: bfloat16 [1024, 128], replicated
- extra_b_out: bfloat16 [128], replicated
- main_ln_gamma: bfloat16 [256], replicated
- main_ln_beta: bfloat16 [256], replicated
- main_w_left: bfloat16 [256, 32], replicated
- main_b_left: bfloat16 [32], replicated
- main_w_right: bfloat16 [256, 32], replicated
- main_b_right: bfloat16 [32], replicated
- main_w_out: bfloat16 [1024, 128], replicated
- main_b_out: bfloat16 [128], replicated
Outputs:
- output 1: float32 [256, 256, 128], P(('data', 'dap'))
- output 2: bfloat16 [3072, 256, 64], P(('data', 'dap'))
- output 3: bfloat16 [512, 256, 256], P(('data', 'dap'))
All inputs are finite; a program needn't handle non-finite values.
Results may differ from the reference program's by a relative error of at most 0.00472692.
Values are sent between devices in bfloat16 or wider.
A program may use at most 1 GiB of HBM per device.

```python
import jax
import jax.numpy as jnp
from jax import lax

NUM_RES = 256
NUM_SEQ = 512
NUM_EXTRA = 3072
MSA_DIM = 256
EXTRA_DIM = 64
OPM_HIDDEN = 32
PAIR_DIM = 128

LN_EPS = 1e-5
NORM_EPS = 1e-3
ROW_BLOCK = min(NUM_RES, 16)


def draw_msa(rng_key, seq_count, msa_width):
    key_profile, key_noise = jax.random.split(rng_key)
    profile = jax.random.normal(key_profile, (1, NUM_RES, msa_width), jnp.float32)
    seq_noise = jax.random.normal(key_noise, (seq_count, NUM_RES, msa_width), jnp.float32)
    return (profile + 0.7 * seq_noise).astype(jnp.bfloat16)


def draw_mask(rng_key, seq_count):
    key_level, key_draw = jax.random.split(rng_key)
    col_level = jax.random.randint(key_level, (1, NUM_RES), 4, 17)
    raw_draws = jax.random.randint(key_draw, (seq_count, NUM_RES), 0, 16)
    kept_mask = (raw_draws < col_level).astype(jnp.int32)
    first_row = jnp.arange(seq_count)[:, None] == 0
    return jnp.where(first_row, 1, kept_mask).astype(jnp.int32)


def draw_weights(rng_key, prefix, msa_width, seq_count):
    weight_keys = jax.random.split(rng_key, 8)
    hidden_sq = OPM_HIDDEN * OPM_HIDDEN
    return {
        prefix + '_ln_gamma': (1.0 + 0.3 * jax.random.normal(weight_keys[0], (msa_width,), jnp.float32)).astype(jnp.bfloat16),
        prefix + '_ln_beta': (0.5 * jax.random.normal(weight_keys[1], (msa_width,), jnp.float32)).astype(jnp.bfloat16),
        prefix + '_w_left': (jax.random.normal(weight_keys[2], (msa_width, OPM_HIDDEN), jnp.float32) * msa_width ** -0.5).astype(jnp.bfloat16),
        prefix + '_b_left': (0.5 * jax.random.normal(weight_keys[3], (OPM_HIDDEN,), jnp.float32)).astype(jnp.bfloat16),
        prefix + '_w_right': (jax.random.normal(weight_keys[4], (msa_width, OPM_HIDDEN), jnp.float32) * msa_width ** -0.5).astype(jnp.bfloat16),
        prefix + '_b_right': (0.5 * jax.random.normal(weight_keys[5], (OPM_HIDDEN,), jnp.float32)).astype(jnp.bfloat16),
        prefix + '_w_out': (jax.random.normal(weight_keys[6], (hidden_sq, PAIR_DIM), jnp.float32) * hidden_sq ** -0.5).astype(jnp.bfloat16),
        prefix + '_b_out': (0.2 * seq_count * jax.random.normal(weight_keys[7], (PAIR_DIM,), jnp.float32)).astype(jnp.bfloat16),
    }


def setup_inputs(seed: int = 0, part: int = 0) -> dict:
    part_keys = jax.random.split(jax.random.fold_in(jax.random.key(seed), part), 5)
    shared_keys = jax.random.split(jax.random.key(seed + 1), 2)
    inputs = {
        'extra_msa': draw_msa(part_keys[0], NUM_EXTRA, EXTRA_DIM),
        'extra_mask': draw_mask(part_keys[1], NUM_EXTRA),
        'main_msa': draw_msa(part_keys[2], NUM_SEQ, MSA_DIM),
        'main_mask': draw_mask(part_keys[3], NUM_SEQ),
        'pair_act': jax.random.normal(part_keys[4], (NUM_RES, NUM_RES, PAIR_DIM), jnp.float32),
    }
    inputs.update(draw_weights(shared_keys[0], 'extra', EXTRA_DIM, NUM_EXTRA))
    inputs.update(draw_weights(shared_keys[1], 'main', MSA_DIM, NUM_SEQ))
    return inputs


def layer_norm(msa_values, ln_gamma, ln_beta):
    as_float = msa_values.astype(jnp.float32)
    row_mean = jnp.mean(as_float, axis=-1, keepdims=True)
    centered = as_float - row_mean
    row_var = jnp.mean(centered * centered, axis=-1, keepdims=True)
    scaled = centered * lax.rsqrt(row_var + LN_EPS)
    return (scaled * ln_gamma.astype(jnp.float32) + ln_beta.astype(jnp.float32)).astype(jnp.bfloat16)


def outer_product_mean(msa_values, mask_int, ln_gamma, ln_beta, w_left, b_left, w_right, b_right, w_out, b_out):
    seq_count, res_count, msa_width = msa_values.shape
    hidden = w_left.shape[1]
    mask_float = mask_int.astype(jnp.float32)
    normed = layer_norm(msa_values, ln_gamma, ln_beta).reshape(seq_count * res_count, msa_width)
    left_acc = jnp.dot(normed, w_left, preferred_element_type=jnp.float32) + b_left.astype(jnp.float32)
    right_acc = jnp.dot(normed, w_right, preferred_element_type=jnp.float32) + b_right.astype(jnp.float32)
    left_proj = (left_acc.reshape(seq_count, res_count, hidden) * mask_float[:, :, None]).astype(jnp.bfloat16)
    right_proj = (right_acc.reshape(seq_count, res_count, hidden) * mask_float[:, :, None]).astype(jnp.bfloat16)
    left_float = left_proj.astype(jnp.float32)
    right_float = right_proj.astype(jnp.float32)
    w_grid = w_out.astype(jnp.float32).reshape(hidden, hidden, -1)
    left_blocks = left_float.reshape(seq_count, res_count // ROW_BLOCK, ROW_BLOCK, hidden).transpose(1, 0, 2, 3)

    def block_term(left_block):
        outer_prod = jnp.einsum('sic,sjd->ijcd', left_block, right_float).astype(jnp.bfloat16).astype(jnp.float32)
        return jnp.einsum('ijcd,cdk->ijk', outer_prod, w_grid)

    pair_sum = lax.map(block_term, left_blocks).reshape(res_count, res_count, -1)
    counts = jnp.dot(mask_float.T, mask_float)
    return (pair_sum + b_out.astype(jnp.float32)) / (NORM_EPS + counts)[:, :, None]


def reference(extra_msa, extra_mask, main_msa, main_mask, pair_act, extra_ln_gamma, extra_ln_beta, extra_w_left, extra_b_left, extra_w_right, extra_b_right, extra_w_out, extra_b_out, main_ln_gamma, main_ln_beta, main_w_left, main_b_left, main_w_right, main_b_right, main_w_out, main_b_out):
    extra_term = outer_product_mean(extra_msa, extra_mask, extra_ln_gamma, extra_ln_beta, extra_w_left, extra_b_left, extra_w_right, extra_b_right, extra_w_out, extra_b_out)
    main_term = outer_product_mean(main_msa, main_mask, main_ln_gamma, main_ln_beta, main_w_left, main_b_left, main_w_right, main_b_right, main_w_out, main_b_out)
    pair_out = pair_act + extra_term + main_term
    return (pair_out, extra_msa, main_msa)
```

```python
import functools

import jax
import jax.numpy as jnp
from jax import lax
from jax.experimental import pallas as pl
from jax.experimental.pallas import tpu as pltpu
from jax.sharding import PartitionSpec as P

LN_EPS = 1e-5
NORM_EPS = 1e-3
NT = (((1,), (1,)), ((), ()))
F32 = jnp.float32
BF16 = jnp.bfloat16
ANY = pl.BlockSpec(memory_space=pl.ANY)
CORE, XBIT, YBIT = 1, 2, 4


def swap(value, bit, size):
    return lax.ppermute(value, 'dap', [(d, d ^ bit) for d in range(size)])


def project_kernel(group, x_ref, mask_ref, gamma_ref, beta_ref, w_ref, bias_ref, a_ref, b_ref):
    rows, chans, seqs = x_ref.shape
    hid = b_ref.shape[0]
    half = group * hid

    def body(step, carry):
        pieces = []
        for part in range(2):
            first = pl.multiple_of(step * 2 * group + part * group, group)
            x = x_ref[pl.ds(first, group)].astype(F32)
            centered = x - jnp.mean(x, axis=1, keepdims=True)
            var = jnp.mean(centered * centered, axis=1, keepdims=True)
            y = centered * lax.rsqrt(var + LN_EPS) * gamma_ref[...][None] + beta_ref[...][None]
            y = y.astype(BF16).reshape(group * chans, seqs)
            z = jnp.dot(w_ref[...], y, preferred_element_type=F32) + bias_ref[...]
            mask = mask_ref[pl.ds(first, group), :]
            left = z[:half].reshape(group, hid, seqs) * mask[:, None, :]
            a_ref[0, pl.ds(pl.multiple_of(first * hid, half), half), :] = left.astype(BF16).reshape(half, seqs)
            pieces.append(z[half:].reshape(hid, group, seqs) * mask[None])
        both = jnp.concatenate(pieces, axis=1).astype(BF16)
        b_ref[:, pl.ds(pl.multiple_of(step * 2 * group, 2 * group), 2 * group), :] = both
        return carry

    lax.fori_loop(0, rows // (2 * group), body, 0)


def project(x, mask_t, gamma, beta, w_left, b_left, w_right, b_right, block=32, group=8):
    res, chans, seqs = x.shape
    hid = w_left.shape[1]
    eye = jnp.eye(group, dtype=BF16)
    w_a = jnp.einsum('gh,mp->gphm', eye, w_left).reshape(group * hid, group * chans)
    w_b = jnp.einsum('gh,mq->qghm', eye, w_right).reshape(group * hid, group * chans)
    w_both = jnp.concatenate([w_a, w_b], axis=0)
    bias = jnp.concatenate([jnp.tile(b_left, group), jnp.repeat(b_right, group)]).astype(F32)
    bias = jnp.broadcast_to(bias[:, None], (2 * group * hid, seqs))
    gamma = jnp.broadcast_to(gamma.astype(F32)[:, None], (chans, seqs))
    beta = jnp.broadcast_to(beta.astype(F32)[:, None], (chans, seqs))
    steps = res // block
    whole = lambda shape: pl.BlockSpec(shape, lambda s: (0,) * len(shape))
    return pl.pallas_call(
        functools.partial(project_kernel, group),
        grid=(steps,),
        in_specs=[
            pl.BlockSpec((block, chans, seqs), lambda s: (s, 0, 0)),
            pl.BlockSpec((block, seqs), lambda s: (s, 0)),
            whole((chans, seqs)), whole((chans, seqs)), whole(w_both.shape), whole(bias.shape),
        ],
        out_specs=[
            pl.BlockSpec((1, block * hid, seqs), lambda s: (s, 0, 0)),
            pl.BlockSpec((hid, block, seqs), lambda s: (0, s, 0)),
        ],
        out_shape=[
            jax.ShapeDtypeStruct((steps, block * hid, seqs), BF16),
            jax.ShapeDtypeStruct((hid, res, seqs), BF16),
        ],
        compiler_params=pltpu.CompilerParams(vmem_limit_bytes=48 << 20),
        cost_estimate=pl.CostEstimate(flops=12 << 30, bytes_accessed=26 << 20, transcendentals=0),
        name='project',
    )(x, mask_t, gamma, beta, w_both, bias)


def outer_kernel(nblk, lens, places, qu, iu, idx_ref, *refs):
    na, nb = len(lens[0]), len(lens[1])
    a_refs, b_refs = refs[:na], refs[na:na + nb]
    w_ref, out_ref, a_v, b_v, o_v, sa, sb = refs[na + nb:]
    rows, hid, _, cols = o_v.shape
    step = pl.program_id(0)
    slot = lax.rem(step, 2)

    def a_copies(st, sl):
        off, out = 0, []
        for t, k in enumerate(lens[0]):
            out.append(pltpu.make_async_copy(a_refs[t].at[idx_ref[t, st]], a_v.at[sl, :, pl.ds(off, k)], sa.at[sl, t]))
            off += k
        return out

    def b_copies():
        off, out = 0, []
        for t, k in enumerate(lens[1]):
            if places is None:
                out.append(pltpu.make_async_copy(b_refs[t], b_v.at[:, :, pl.ds(off, k)], sb.at[t]))
                off += k
            else:
                width = cols // nb
                at = pl.multiple_of((idx_ref[na, 0] ^ places[t]) * width, width)
                out.append(pltpu.make_async_copy(b_refs[t], b_v.at[:, pl.ds(at, width), :], sb.at[t]))
        return out

    @pl.when(step == 0)
    def _():
        for c in a_copies(0, 0) + b_copies():
            c.start()
        for c in b_copies():
            c.wait()

    for c in a_copies(step, slot):
        c.wait()

    @pl.when(step + 1 < nblk)
    def _():
        for c in a_copies(step + 1, 1 - slot):
            c.start()

    def q_body(g, carry):
        for u in range(qu):
            q = g * qu + u
            o = lax.dot_general(a_v[slot], b_v[q], NT, preferred_element_type=F32)
            o_v[:, q] = o.astype(BF16).reshape(rows, hid, cols)
        return carry

    lax.fori_loop(0, hid // qu, q_body, 0)

    def i_body(g, carry):
        for u in range(iu):
            i = g * iu + u
            r = jnp.dot(w_ref[...], o_v[i].reshape(hid * hid, cols), preferred_element_type=F32)
            out_ref[i] = r.astype(out_ref.dtype)
        return carry

    lax.fori_loop(0, rows // iu, i_body, 0)


def outer(idx, a_list, b_list, w_out, nblk, cols, out_dtype, places=None, qu=8, iu=8):
    hid = b_list[0].shape[0]
    rows = a_list[0].shape[1] // hid
    depth = sum(a.shape[2] for a in a_list)
    chans = w_out.shape[1]
    w_t = w_out.reshape(hid, hid, chans).transpose(2, 1, 0).reshape(chans, hid * hid)
    lens = (tuple(a.shape[2] for a in a_list), tuple(b.shape[2] for b in b_list))
    flops = 2 * nblk * rows * hid * hid * cols * (depth + chans)
    return pl.pallas_call(
        functools.partial(outer_kernel, nblk, lens, places, qu, iu),
        grid_spec=pltpu.PrefetchScalarGridSpec(
            num_scalar_prefetch=1,
            grid=(nblk,),
            in_specs=[ANY] * (len(a_list) + len(b_list)) + [pl.BlockSpec(w_t.shape, lambda s, i: (0, 0))],
            out_specs=pl.BlockSpec((rows, chans, cols), lambda s, i: (s, 0, 0)),
            scratch_shapes=[
                pltpu.VMEM((2, rows * hid, depth), BF16),
                pltpu.VMEM((hid, cols, depth), BF16),
                pltpu.VMEM((rows, hid, hid, cols), BF16),
                pltpu.SemaphoreType.DMA((2, len(a_list))),
                pltpu.SemaphoreType.DMA((len(b_list),)),
            ],
        ),
        out_shape=jax.ShapeDtypeStruct((nblk * rows, chans, cols), out_dtype),
        compiler_params=pltpu.CompilerParams(vmem_limit_bytes=60 << 20),
        cost_estimate=pl.CostEstimate(flops=flops, bytes_accessed=32 << 20, transcendentals=0),
        name='outer',
    )(idx, *a_list, *b_list, w_t)


def combine_kernel(count, *refs):
    parts = refs[:count]
    main_ref, z_ref, den_e_ref, den_m_ref, bias_e_ref, bias_m_ref, out_ref = refs[count:]
    for i in range(out_ref.shape[0]):
        extra = parts[0][i].astype(F32)
        for part in parts[1:]:
            extra = extra + part[i].astype(F32)
        extra = (extra + bias_e_ref[...]) / den_e_ref[pl.ds(i, 1), :]
        main = (main_ref[i] + bias_m_ref[...]) / den_m_ref[pl.ds(i, 1), :]
        out_ref[i] = z_ref[i] + (extra + main).T


def combine(parts, main, z, den_e, den_m, bias_e, bias_m, block=8):
    rows, cols, chans = z.shape
    t_spec = lambda: pl.BlockSpec((block, chans, cols), lambda s: (s, 0, 0))
    z_spec = lambda: pl.BlockSpec((block, cols, chans), lambda s: (s, 0, 0))
    d_spec = lambda: pl.BlockSpec((block, cols), lambda s: (s, 0))
    c_spec = lambda: pl.BlockSpec((chans, cols), lambda s: (0, 0))
    wide = lambda b: jnp.broadcast_to(b.astype(F32)[:, None], (chans, cols))
    return pl.pallas_call(
        functools.partial(combine_kernel, len(parts)),
        grid=(rows // block,),
        in_specs=[t_spec() for _ in parts] + [t_spec(), z_spec(), d_spec(), d_spec(), c_spec(), c_spec()],
        out_specs=z_spec(),
        out_shape=jax.ShapeDtypeStruct(z.shape, F32),
        cost_estimate=pl.CostEstimate(flops=1 << 24, bytes_accessed=20 << 20, transcendentals=0),
        name='combine',
    )(*parts, main, z, den_e, den_m, wide(bias_e), wide(bias_m))


def layer_norm(value, gamma, beta):
    as_float = value.astype(F32)
    mean = jnp.mean(as_float, axis=-1, keepdims=True)
    centered = as_float - mean
    var = jnp.mean(centered * centered, axis=-1, keepdims=True)
    return (centered * lax.rsqrt(var + LN_EPS) * gamma.astype(F32) + beta.astype(F32)).astype(BF16)


def denominators(mask, mask_rows):
    counts = jnp.einsum('si,sj->ij', mask_rows.astype(BF16), mask.astype(BF16), preferred_element_type=F32)
    return NORM_EPS + counts


def solution(mesh):
    size = mesh.shape['dap']
    value_spec = P('data', 'dap', None)
    mask_spec = P('data', None)
    row_spec = P(('data', 'dap'), None, None)

    def local_program(extra_block, extra_mask, main_block, main_mask, pair_rows, eg, eb, ewl, ebl, ewr, ebr, ewo, ebo, mg, mb, mwl, mbl, mwr, mbr, mwo, mbo):
        me = lax.axis_index('dap')
        core, chip = lax.rem(me, 2), me // 2
        rows = extra_block.shape[1]
        hid = ewl.shape[1]

        seqs = extra_block.shape[0] // size
        chans = extra_block.shape[2]
        turned = extra_block.transpose(1, 2, 0).reshape(rows, chans, size, seqs).transpose(2, 0, 1, 3)
        extra_t = lax.all_to_all(turned, 'dap', 0, 0, tiled=True).reshape(size * rows, chans, seqs)
        extra_out = extra_t.transpose(2, 0, 1)

        mask_rows_m = lax.dynamic_slice_in_dim(main_mask, me * rows, rows, axis=1)
        mask_rows_e = lax.dynamic_slice_in_dim(extra_mask, me * rows, rows, axis=1)
        den_m = denominators(main_mask, mask_rows_m)
        den_e = denominators(extra_mask, mask_rows_e)
        normed = layer_norm(main_block, mg, mb)
        mask_m = mask_rows_m.astype(F32).T
        a_m = jnp.einsum('sim,mp->ips', normed, mwl, preferred_element_type=F32) + mbl.astype(F32)[None, :, None]
        a_m = (a_m * mask_m[:, None, :]).astype(BF16).reshape(1, rows * hid, -1)
        b_m = jnp.einsum('sim,mq->qis', normed, mwr, preferred_element_type=F32) + mbr.astype(F32)[:, None, None]
        b_m = (b_m * mask_m[None]).astype(BF16)

        extra_t, main_block, b_m = lax.optimization_barrier((extra_t, main_block, b_m))
        main_out = lax.all_to_all(main_block, 'dap', 0, 1, tiled=True)
        b_x, b_y = swap(b_m, XBIT, size), swap(b_m, YBIT, size)
        cut = hid // 2
        b_d = jnp.concatenate([swap(b_x[:cut], YBIT, size), swap(b_y[cut:], XBIT, size)], axis=0)
        b_parts = [b_m, b_x, b_y, b_d]
        b_parts = b_parts + [swap(part, CORE, size) for part in b_parts]
        places = (0, XBIT, YBIT, XBIT | YBIT, CORE, CORE | XBIT, CORE | YBIT, CORE | XBIT | YBIT)

        mask_seq = lax.dynamic_slice_in_dim(extra_mask, me * seqs, seqs, axis=0).astype(F32).T
        a_e, b_e = project(extra_t, mask_seq, eg, eb, ewl, ebl, ewr, ebr)
        a_split = a_e.reshape(size // 2, 2, rows * hid, seqs)
        a_give = lax.dynamic_index_in_dim(a_split, 1 - core, axis=1, keepdims=False)
        a_sib, b_sib = swap(a_give, CORE, size), swap(b_e, CORE, size)
        order = chip ^ jnp.array([3, 1, 2, 0], jnp.int32)
        idx = jnp.stack([order * 2 + core, order]).astype(jnp.int32)
        part = outer(idx, [a_e, a_sib], [b_e, b_sib], ewo, size // 2, size * rows, BF16)
        part = part.reshape(size // 2, rows, part.shape[1], part.shape[2])
        got = [swap(part[t], 2 * k, size) for t, k in enumerate((3, 1, 2))]

        idx_m = jnp.stack([jnp.zeros((), jnp.int32), me.astype(jnp.int32)])[:, None]
        main_sum = outer(idx_m, [a_m], b_parts, mwo, 1, size * rows, F32, places=places)
        pair_out = combine([part[3]] + got, main_sum, pair_rows, den_e, den_m, ebo, mbo)
        return pair_out, extra_out, main_out

    in_specs = (value_spec, mask_spec, value_spec, mask_spec, row_spec) + (P(),) * 16
    return jax.shard_map(local_program, mesh=mesh, in_specs=in_specs, out_specs=(row_spec, row_spec, row_spec), check_vma=False)
```

```python
import functools

import jax
import jax.numpy as jnp
from jax import lax
from jax.experimental import pallas as pl
from jax.experimental.pallas import tpu as pltpu
from jax.sharding import PartitionSpec as P


LN_EPS = 1e-5
NORM_EPS = 1e-3
NT = (((1,), (1,)), ((), ()))
F32 = jnp.float32
BF16 = jnp.bfloat16
ANY = pl.BlockSpec(memory_space=pl.ANY)
CORE, XBIT, YBIT = 1, 2, 4
LANES = 128
NEAR, REST = (2, 4, 3, 5), (6, 7, 1, 0)


def swap(value, bit, size):
    return lax.ppermute(value, 'dap', [(d, d ^ bit) for d in range(size)])


def turn_kernel(ks, me_ref, x_ref, *refs):
    outs, (v, s_in, s_out) = refs[:len(ks)], refs[len(ks):]
    seqs = v.shape[3]
    loads = [
        pltpu.make_async_copy(x_ref.at[:, :, pl.ds(pl.multiple_of((me_ref[0] ^ k) * seqs, LANES), seqs)], v.at[t], s_in.at[t])
        for t, k in enumerate(ks)
    ]
    stores = [pltpu.make_async_copy(v.at[t], out, s_out.at[t]) for t, out in enumerate(outs)]
    for c in loads:
        c.start()
    for load, save in zip(loads, stores):
        load.wait()
        save.start()
    for c in stores:
        c.wait()


def turn(me, x, ks, size):
    rows, chans, total = x.shape
    seqs = total // size
    return pl.pallas_call(
        functools.partial(turn_kernel, ks),
        grid_spec=pltpu.PrefetchScalarGridSpec(
            num_scalar_prefetch=1,
            grid=(1,),
            in_specs=[ANY],
            out_specs=[ANY] * len(ks),
            scratch_shapes=[
                pltpu.VMEM((len(ks), rows, chans, seqs), x.dtype),
                pltpu.SemaphoreType.DMA((len(ks),)),
                pltpu.SemaphoreType.DMA((len(ks),)),
            ],
        ),
        out_shape=[jax.ShapeDtypeStruct((rows, chans, seqs), x.dtype) for _ in ks],
        cost_estimate=pl.CostEstimate(flops=1 << 24, bytes_accessed=4 << 20, transcendentals=0),
        name='turn',
    )(me, x)


def turn_out_kernel(ks, me_ref, *refs):
    x_refs, (out_ref, in_v, out_v) = refs[:len(ks)], refs[len(ks):]
    rows, lead = x_refs[0].shape[:2]
    for k, ref in zip(ks, x_refs):
        in_v[pl.ds(pl.multiple_of((me_ref[0] ^ k) * rows, rows), rows)] = ref[...].astype(F32)
    for c in range(lead):
        out_v[:, c, :] = in_v[:, c, :].T
    out_ref[...] = out_v[...].astype(BF16)


def turn_out(me, blocks, lead=8):
    ks = tuple(sorted(blocks))
    rows, chans, seqs = blocks[ks[0]].shape
    res = rows * len(ks)
    return pl.pallas_call(
        functools.partial(turn_out_kernel, ks),
        grid_spec=pltpu.PrefetchScalarGridSpec(
            num_scalar_prefetch=1,
            grid=(seqs // LANES, chans // lead),
            in_specs=[pl.BlockSpec((rows, lead, LANES), lambda k, c, i: (0, c, k)) for _ in ks],
            out_specs=pl.BlockSpec((LANES, lead, res), lambda k, c, i: (k, c, 0)),
            scratch_shapes=[pltpu.VMEM((res, lead, LANES), F32), pltpu.VMEM((LANES, lead, res), F32)],
        ),
        out_shape=jax.ShapeDtypeStruct((seqs, chans, res), BF16),
        cost_estimate=pl.CostEstimate(flops=1 << 24, bytes_accessed=25 << 20, transcendentals=0),
        name='turn_out',
    )(me, *[blocks[k] for k in ks])


def project_kernel(group, idx_ref, *refs):
    count = len(refs) - 12
    x_refs = refs[:count]
    mask_ref, gamma_ref, beta_ref, w_ref, bias_ref, own_ref, sib_ref, b_ref, x_v, a_v, s_in, s_out = refs[count:]
    rows, chans, seqs = x_v.shape[1:]
    hid = b_ref.shape[1]
    half = group * hid
    block = pl.program_id(0)
    slot = lax.rem(block, 2)
    loads = [pltpu.make_async_copy(ref, x_v.at[t], s_in.at[t]) for t, ref in enumerate(x_refs)]
    targets = [own_ref.at[t] for t in range(count // 2)] + [sib_ref.at[t] for t in range(count // 2)]
    saves = [pltpu.make_async_copy(a_v.at[t % 2], target, s_out.at[t % 2]) for t, target in enumerate(targets)]

    @pl.when(block == 0)
    def _():
        for c in loads:
            c.start()

    for t in range(count):
        @pl.when(block == t)
        def _(t=t):
            loads[t].wait()
            if t >= 2:
                saves[t - 2].wait()

    def body(step, carry):
        pieces = []
        for part in range(2):
            first = pl.multiple_of(step * 2 * group + part * group, group)
            x = x_v[block, pl.ds(first, group)].astype(F32)
            centered = x - jnp.mean(x, axis=1, keepdims=True)
            var = jnp.mean(centered * centered, axis=1, keepdims=True)
            y = centered * lax.rsqrt(var + LN_EPS) * gamma_ref[...][None] + beta_ref[...][None]
            y = y.astype(BF16).reshape(group * chans, seqs)
            z = jnp.dot(w_ref[...], y, preferred_element_type=F32) + bias_ref[...]
            mask = mask_ref[pl.ds(first, group), :]
            left = z[:half].reshape(group, hid, seqs) * mask[:, None, :]
            a_v[slot, pl.ds(pl.multiple_of(first * hid, half), half), :] = left.astype(BF16).reshape(half, seqs)
            pieces.append(z[half:].reshape(hid, group, seqs) * mask[None])
        both = jnp.concatenate(pieces, axis=1).astype(BF16)
        b_ref[0, :, pl.ds(pl.multiple_of(step * 2 * group, 2 * group), 2 * group), :] = both
        return carry

    lax.fori_loop(0, rows // (2 * group), body, 0)
    for t in range(count):
        @pl.when(block == t)
        def _(t=t):
            saves[t].start()
            if t == count - 1:
                for c in saves[t - 1:]:
                    c.wait()


def project_weights(w_left, b_left, w_right, b_right, seqs, group=8):
    chans, hid = w_left.shape
    eye = jnp.eye(group, dtype=BF16)
    w_a = jnp.einsum('gh,mp->gphm', eye, w_left).reshape(group * hid, group * chans)
    w_b = jnp.einsum('gh,mq->qghm', eye, w_right).reshape(group * hid, group * chans)
    w_both = jnp.concatenate([w_a, w_b], axis=0)
    bias = jnp.concatenate([jnp.tile(b_left, group), jnp.repeat(b_right, group)]).astype(F32)
    return w_both, jnp.broadcast_to(bias[:, None], (2 * group * hid, seqs))


def project(idx, blocks, mask_t, gamma, beta, w_both, bias, hid, group=8):
    count = len(blocks)
    rows, chans, seqs = blocks[0].shape
    whole = lambda v: pl.BlockSpec(v.shape, lambda s, i: (0,) * v.ndim)
    return pl.pallas_call(
        functools.partial(project_kernel, group),
        grid_spec=pltpu.PrefetchScalarGridSpec(
            num_scalar_prefetch=1,
            grid=(count,),
            in_specs=[ANY] * count + [
                pl.BlockSpec((rows, seqs), lambda s, i: (i[s], 0)),
                whole(gamma), whole(beta), whole(w_both), whole(bias),
            ],
            out_specs=[ANY, ANY, pl.BlockSpec((1, hid, rows, seqs), lambda s, i: (s, 0, 0, 0))],
            scratch_shapes=[
                pltpu.VMEM((count, rows, chans, seqs), BF16),
                pltpu.VMEM((2, rows * hid, seqs), BF16),
                pltpu.SemaphoreType.DMA((count,)),
                pltpu.SemaphoreType.DMA((2,)),
            ],
        ),
        out_shape=[
            jax.ShapeDtypeStruct((count // 2, rows * hid, seqs), BF16),
            jax.ShapeDtypeStruct((count // 2, rows * hid, seqs), BF16),
            jax.ShapeDtypeStruct((count, hid, rows, seqs), BF16),
        ],
        compiler_params=pltpu.CompilerParams(vmem_limit_bytes=48 << 20),
        cost_estimate=pl.CostEstimate(flops=6 << 30, bytes_accessed=13 << 20, transcendentals=0),
        name='project',
    )(idx, *blocks, mask_t, gamma, beta, w_both, bias)


def outer_rows(a, b_v, o_v, qu, ready=None):
    rows, hid, _, cols = o_v.shape

    def q_body(g, carry):
        if ready is not None:
            ready(g)
        for u in range(qu):
            q = g * qu + u
            o = lax.dot_general(a[...], b_v[q], NT, preferred_element_type=F32)
            o_v[:, q] = o.astype(BF16).reshape(rows, hid, cols)
        return carry

    lax.fori_loop(0, hid // qu, q_body, 0)


def weigh_rows(w_ref, o_v, iu, store):
    rows, hid, _, cols = o_v.shape

    def i_body(g, carry):
        for u in range(iu):
            i = g * iu + u
            store(i, jnp.dot(w_ref[...], o_v[i].reshape(hid * hid, cols), preferred_element_type=F32))
        return carry

    lax.fori_loop(0, rows // iu, i_body, 0)


SET_A, SET_B = (0, 2, 4, 1, 3, 5), (6, 7)


def extra_kernel(qu, iu, me_ref, *refs):
    (a_a, a_a_sib, a_b, a_b_sib), b_refs = refs[:4], refs[4:8]
    w_ref, sx, sy, kx, ky, own, a_v, b_v, o_v, r_v, sa, sb, so = refs[8:]
    step = pl.program_id(0)
    slot = lax.rem(step, 2)
    half = kx.shape[0]
    lo, hi = pl.ds(0, half), pl.ds(half, half)
    depth = a_a.shape[2]
    width = b_refs[0].shape[2]

    def a_copies(t):
        pair, at = (((a_b, a_b_sib), 0), ((a_a, a_a_sib), 1), ((a_a, a_a_sib), 2), ((a_a, a_a_sib), 0))[t]
        return [
            pltpu.make_async_copy(ref.at[at], a_v.at[t % 2, :, pl.ds(n * depth, depth)], sa.at[t % 2, n])
            for n, ref in enumerate(pair)
        ]

    def b_copies(g):
        out = []
        qs = pl.ds(g * qu, qu)
        pieces = [(n, ref, t, k) for n, (ref, ks) in enumerate(zip(b_refs, (SET_A, SET_A, SET_B, SET_B))) for t, k in enumerate(ks)]
        for m, (n, ref, t, k) in enumerate(pieces):
            k = k ^ CORE if n % 2 else k
            js = pl.ds(pl.multiple_of((me_ref[0] ^ k) * width, width), width)
            out.append(pltpu.make_async_copy(ref.at[t, qs], b_v.at[qs, js, pl.ds(n % 2 * depth, depth)], sb.at[g, m]))
        return out

    def out_copies(t):
        lower, upper = ((sx.at[0], sy.at[0]), (sx.at[1], kx), (ky, sy.at[1]), (own.at[lo], own.at[hi]))[t]
        sl = t % 2
        return [
            pltpu.make_async_copy(r_v.at[sl, lo], lower, so.at[sl, 0]),
            pltpu.make_async_copy(r_v.at[sl, hi], upper, so.at[sl, 1]),
        ]

    @pl.when(step == 0)
    def _():
        for c in a_copies(0):
            c.start()
        for g in range(b_v.shape[0] // qu):
            for c in b_copies(g):
                c.start()

    for t in range(4):
        @pl.when(step == t)
        def _(t=t):
            for c in a_copies(t):
                c.wait()
            if t < 3:
                for c in a_copies(t + 1):
                    c.start()

    def ready(g):
        @pl.when(step == 0)
        def _():
            for c in b_copies(g):
                c.wait()

    outer_rows(a_v.at[slot], b_v, o_v, qu, ready)
    for t in range(2, 4):
        @pl.when(step == t)
        def _(t=t):
            for c in out_copies(t - 2):
                c.wait()

    def store(i, r):
        r_v[slot, i] = r.astype(BF16)

    weigh_rows(w_ref, o_v, iu, store)
    for t in range(4):
        @pl.when(step == t)
        def _(t=t):
            for c in out_copies(t):
                c.start()
            if t == 3:
                for c in out_copies(2) + out_copies(3):
                    c.wait()


def turn_weights(w_out, hid):
    return w_out.reshape(hid, hid, -1).transpose(2, 1, 0).reshape(-1, hid * hid)


def extra_parts(me, a_parts, b_parts, w_t, cols, qu=8, iu=8):
    hid, depth = b_parts[0].shape[1], 2 * b_parts[0].shape[3]
    rows = a_parts[0].shape[1] // hid
    chans = w_t.shape[0]
    half = rows // 2
    part = lambda *lead: jax.ShapeDtypeStruct(lead + (chans, cols), BF16)
    return pl.pallas_call(
        functools.partial(extra_kernel, qu, iu),
        grid_spec=pltpu.PrefetchScalarGridSpec(
            num_scalar_prefetch=1,
            grid=(4,),
            in_specs=[ANY] * 8 + [pl.BlockSpec(w_t.shape, lambda s, i: (0, 0))],
            out_specs=[ANY] * 5,
            scratch_shapes=[
                pltpu.VMEM((2, rows * hid, depth), BF16),
                pltpu.VMEM((hid, cols, depth), BF16),
                pltpu.VMEM((rows, hid, hid, cols), BF16),
                pltpu.VMEM((2, rows, chans, cols), BF16),
                pltpu.SemaphoreType.DMA((2, 2)),
                pltpu.SemaphoreType.DMA((hid // qu, 16)),
                pltpu.SemaphoreType.DMA((2, 2)),
            ],
        ),
        out_shape=[part(2, half), part(2, half), part(half), part(half), part(rows)],
        compiler_params=pltpu.CompilerParams(vmem_limit_bytes=60 << 20),
        cost_estimate=pl.CostEstimate(flops=60 << 30, bytes_accessed=32 << 20, transcendentals=0),
        name='extra_outer',
    )(me, *a_parts, *b_parts, w_t)


def main_kernel(places, qu, iu, idx_ref, a_ref, *refs):
    b_refs = refs[:len(places)]
    w_ref, bias_ref, den_ref, z_ref, out_ref, b_v, o_v, sb = refs[len(places):]
    copies = []
    for t, (ref, (k, first)) in enumerate(zip(b_refs, places)):
        count, width = ref.shape[:2]
        at = pl.multiple_of((idx_ref[0] ^ k) * width, width)
        copies.append(pltpu.make_async_copy(ref, b_v.at[pl.ds(first, count), pl.ds(at, width), :], sb.at[t]))
    for c in copies:
        c.start()
    for c in copies:
        c.wait()
    outer_rows(a_ref, b_v, o_v, qu)

    def store(i, r):
        out_ref[i] = z_ref[i] + ((r + bias_ref[...]) / den_ref[pl.ds(i, 1), :]).T

    weigh_rows(w_ref, o_v, iu, store)


def main_rows(me, a, b_parts, places, w_t, bias, den, z, qu=8, iu=8):
    hid, _, depth = b_parts[0].shape
    rows, cols, _ = z.shape
    whole = lambda v: pl.BlockSpec(v.shape, lambda s, i: (0,) * v.ndim)
    return pl.pallas_call(
        functools.partial(main_kernel, places, qu, iu),
        grid_spec=pltpu.PrefetchScalarGridSpec(
            num_scalar_prefetch=1,
            grid=(1,),
            in_specs=[whole(a)] + [ANY] * len(b_parts) + [whole(w_t), whole(bias), whole(den), whole(z)],
            out_specs=whole(z),
            scratch_shapes=[
                pltpu.VMEM((hid, cols, depth), BF16),
                pltpu.VMEM((rows, hid, hid, cols), BF16),
                pltpu.SemaphoreType.DMA((len(b_parts),)),
            ],
        ),
        out_shape=jax.ShapeDtypeStruct(z.shape, F32),
        compiler_params=pltpu.CompilerParams(vmem_limit_bytes=60 << 20),
        cost_estimate=pl.CostEstimate(flops=12 << 30, bytes_accessed=20 << 20, transcendentals=0),
        name='main_outer',
    )(me, a, *b_parts, w_t, bias, den, z)


def combine_kernel(own_ref, rx_ref, ry_ref, tx_ref, ty_ref, base_ref, den_ref, bias_ref, out_ref):
    step = pl.program_id(0)

    def add(first, second):
        for i in range(out_ref.shape[0]):
            total = own_ref[i].astype(F32) + first[0, i].astype(F32) + second[i].astype(F32)
            out_ref[i] = base_ref[i] + ((total + bias_ref[...]) / den_ref[pl.ds(i, 1), :]).T

    @pl.when(step < pl.num_programs(0) // 2)
    def _():
        add(rx_ref, ty_ref)

    @pl.when(step >= pl.num_programs(0) // 2)
    def _():
        add(ry_ref, tx_ref)


def combine(own, rx, ry, tx, ty, base, den, bias, block=8):
    rows, cols, chans = base.shape
    mid = rows // block // 2
    lower = lambda s: jnp.minimum(s, mid - 1)
    upper = lambda s: jnp.maximum(s - mid, 0)
    flat = lambda: pl.BlockSpec((block, cols, chans), lambda s: (s, 0, 0))
    return pl.pallas_call(
        combine_kernel,
        grid=(2 * mid,),
        in_specs=[
            pl.BlockSpec((block, chans, cols), lambda s: (s, 0, 0)),
            pl.BlockSpec((1, block, chans, cols), lambda s: (1, lower(s), 0, 0)),
            pl.BlockSpec((1, block, chans, cols), lambda s: (1, upper(s), 0, 0)),
            pl.BlockSpec((block, chans, cols), lambda s: (upper(s), 0, 0)),
            pl.BlockSpec((block, chans, cols), lambda s: (lower(s), 0, 0)),
            flat(),
            pl.BlockSpec((block, cols), lambda s: (s, 0)),
            pl.BlockSpec((chans, cols), lambda s: (0, 0)),
        ],
        out_specs=flat(),
        out_shape=jax.ShapeDtypeStruct(base.shape, F32),
        cost_estimate=pl.CostEstimate(flops=1 << 24, bytes_accessed=15 << 20, transcendentals=0),
        name='combine',
    )(own, rx, ry, tx, ty, base, den, bias)


def assemble_kernel(ref, out_ref):
    width = ref.shape[2]
    for d in range(ref.shape[0]):
        out_ref[:, d * width:(d + 1) * width, :] = ref[d]


def assemble(value, block=8):
    srcs, seqs, width, chans = value.shape
    return pl.pallas_call(
        assemble_kernel,
        grid=(seqs // block,),
        in_specs=[pl.BlockSpec((srcs, block, width, chans), lambda s: (0, s, 0, 0))],
        out_specs=pl.BlockSpec((block, srcs * width, chans), lambda s: (s, 0, 0)),
        out_shape=jax.ShapeDtypeStruct((seqs, srcs * width, chans), value.dtype),
        cost_estimate=pl.CostEstimate(flops=1 << 24, bytes_accessed=16 << 20, transcendentals=0),
        name='assemble',
    )(value)


def layer_norm(value, gamma, beta):
    as_float = value.astype(F32)
    mean = jnp.mean(as_float, axis=-1, keepdims=True)
    centered = as_float - mean
    var = jnp.mean(centered * centered, axis=-1, keepdims=True)
    return (centered * lax.rsqrt(var + LN_EPS) * gamma.astype(F32) + beta.astype(F32)).astype(BF16)


def denominators(mask, mask_rows):
    counts = jnp.einsum('si,sj->ij', mask_rows.astype(BF16), mask.astype(BF16), preferred_element_type=F32)
    return NORM_EPS + counts


def solution(mesh):
    size = mesh.shape['dap']
    value_spec = P('data', 'dap', None)
    mask_spec = P('data', None)
    row_spec = P(('data', 'dap'), None, None)

    def local_program(extra_block, extra_mask, main_block, main_mask, pair_rows, eg, eb, ewl, ebl, ewr, ebr, ewo, ebo, mg, mb, mwl, mbl, mwr, mbr, mwo, mbo):
        me = lax.axis_index('dap')
        rows = extra_block.shape[1]
        hid = ewl.shape[1]

        seqs = extra_block.shape[0] // size
        cols = size * rows
        minor = extra_block.transpose(1, 2, 0)
        me1 = me.astype(jnp.int32)[None]
        turned = dict(zip(NEAR, turn(me1, minor, NEAR, size)))
        turned.update(zip(REST, turn(me1, minor, REST, size)))
        blocks = {0: turned[0]}
        for k in NEAR:
            blocks[k] = swap(turned[k], k, size)
        blocks[1] = swap(turned[1], CORE, size)
        near, far = lax.optimization_barrier(([blocks[k] for k in NEAR], [turned[6], turned[7]]))
        blocks.update(zip(NEAR, near))
        for k, value in zip((6, 7), far):
            blocks[k] = swap(value, k, size)

        mask_rows_m = lax.dynamic_slice_in_dim(main_mask, me * rows, rows, axis=1)
        mask_rows_e = lax.dynamic_slice_in_dim(extra_mask, me * rows, rows, axis=1)
        den_m = denominators(main_mask, mask_rows_m)
        den_e = denominators(extra_mask, mask_rows_e)
        normed = layer_norm(main_block, mg, mb)
        mask_m = mask_rows_m.astype(F32).T
        a_m = jnp.einsum('sim,mp->ips', normed, mwl, preferred_element_type=F32) + mbl.astype(F32)[None, :, None]
        a_m = (a_m * mask_m[:, None, :]).astype(BF16).reshape(rows * hid, -1)
        b_m = jnp.einsum('sim,mq->qis', normed, mwr, preferred_element_type=F32) + mbr.astype(F32)[:, None, None]
        b_m = (b_m * mask_m[None]).astype(BF16)

        wide = lambda v, n: jnp.broadcast_to(v.astype(F32)[:, None], (v.shape[0], n))
        mask_seq = lax.dynamic_slice_in_dim(extra_mask, me * seqs, seqs, axis=0).astype(F32).T
        w_both, bias = project_weights(ewl, ebl, ewr, ebr, seqs)
        gamma, beta = wide(eg, seqs), wide(eb, seqs)
        idx_a, idx_b = [(me ^ jnp.array(ks, jnp.int32)).astype(jnp.int32) for ks in (SET_A, SET_B)]
        w_e, w_m = turn_weights(ewo, hid), turn_weights(mwo, hid)
        bias_e, bias_m = wide(ebo, cols), wide(mbo, cols)

        a_a, a_a_give, b_a = project(idx_a, [blocks[k] for k in SET_A], mask_seq, gamma, beta, w_both, bias, hid)
        a_a_sib, b_a_sib = swap(a_a_give, CORE, size), swap(b_a, CORE, size)

        blocks[6], blocks[7], main_moved, b_m = lax.optimization_barrier((blocks[6], blocks[7], main_block, b_m))
        main_moved = lax.all_to_all(main_moved, 'dap', 0, 0, tiled=True).reshape(size, -1, rows, main_block.shape[2])
        b_x, b_y = swap(b_m, XBIT, size), swap(b_m, YBIT, size)
        mid = hid // 2
        b_d = [swap(b_x[:mid], YBIT, size), swap(b_y[mid:], XBIT, size)]
        b_parts = [b_m, b_x, b_y]
        b_parts = b_parts + [swap(part, CORE, size) for part in b_parts]
        b_parts = b_parts + b_d + [swap(part, CORE, size) for part in b_d]
        places = ((0, 0), (XBIT, 0), (YBIT, 0), (CORE, 0), (CORE | XBIT, 0), (CORE | YBIT, 0))
        places = places + ((XBIT | YBIT, 0), (XBIT | YBIT, mid), (CORE | XBIT | YBIT, 0), (CORE | XBIT | YBIT, mid))

        a_b, a_b_give, b_b = project(idx_b, [blocks[k] for k in SET_B], mask_seq, gamma, beta, w_both, bias, hid)
        a_b_sib, b_b_sib = swap(a_b_give, CORE, size), swap(b_b, CORE, size)
        sx, sy, kx, ky, own = extra_parts(me1, (a_a, a_a_sib, a_b, a_b_sib), (b_a, b_a_sib, b_b, b_b_sib), w_e, cols)
        rx, ry = swap(sx, XBIT, size), swap(sy, YBIT, size)
        kx = (kx.astype(F32) + ry[0].astype(F32)).astype(BF16)
        ky = (ky.astype(F32) + rx[0].astype(F32)).astype(BF16)
        tx, ty = swap(kx, XBIT, size), swap(ky, YBIT, size)

        base = main_rows(me1, a_m, b_parts, places, w_m, bias_m, den_m, pair_rows)
        main_out = assemble(main_moved)
        extra_out = turn_out(me1, blocks).transpose(0, 2, 1)
        pair_out = combine(own, rx, ry, tx, ty, base, den_e, bias_e)
        return pair_out, extra_out, main_out

    in_specs = (value_spec, mask_spec, value_spec, mask_spec, row_spec) + (P(),) * 16
    return jax.shard_map(local_program, mesh=mesh, in_specs=in_specs, out_specs=(row_spec, row_spec, row_spec), check_vma=False)
```

```python
import functools

import jax
import jax.numpy as jnp
from jax import lax
from jax.experimental import pallas as pl
from jax.experimental.pallas import tpu as pltpu
from jax.sharding import PartitionSpec as P


LN_EPS = 1e-5
NORM_EPS = 1e-3
NT = (((1,), (1,)), ((), ()))
F32 = jnp.float32
BF16 = jnp.bfloat16
ANY = pl.BlockSpec(memory_space=pl.ANY)
CORE, XBIT, YBIT = 1, 2, 4
LANES = 128
NEAR, REST = (2, 4, 3, 5), (6, 7, 1, 0)


def swap(value, bit, size):
    return lax.ppermute(value, 'dap', [(d, d ^ bit) for d in range(size)])


def turn_kernel(ks, me_ref, x_ref, *refs):
    outs, (v, s_in, s_out) = refs[:len(ks)], refs[len(ks):]
    seqs = v.shape[3]
    loads = [
        pltpu.make_async_copy(x_ref.at[:, :, pl.ds(pl.multiple_of((me_ref[0] ^ k) * seqs, LANES), seqs)], v.at[t], s_in.at[t])
        for t, k in enumerate(ks)
    ]
    stores = [pltpu.make_async_copy(v.at[t], out, s_out.at[t]) for t, out in enumerate(outs)]
    for c in loads:
        c.start()
    for load, save in zip(loads, stores):
        load.wait()
        save.start()
    for c in stores:
        c.wait()


def turn(me, x, ks, size):
    rows, chans, total = x.shape
    seqs = total // size
    return pl.pallas_call(
        functools.partial(turn_kernel, ks),
        grid_spec=pltpu.PrefetchScalarGridSpec(
            num_scalar_prefetch=1,
            grid=(1,),
            in_specs=[ANY],
            out_specs=[ANY] * len(ks),
            scratch_shapes=[
                pltpu.VMEM((len(ks), rows, chans, seqs), x.dtype),
                pltpu.SemaphoreType.DMA((len(ks),)),
                pltpu.SemaphoreType.DMA((len(ks),)),
            ],
        ),
        out_shape=[jax.ShapeDtypeStruct((rows, chans, seqs), x.dtype) for _ in ks],
        cost_estimate=pl.CostEstimate(flops=1 << 24, bytes_accessed=4 << 20, transcendentals=0),
        name='turn',
    )(me, x)


def turn_out_kernel(ks, me_ref, *refs):
    x_refs, (out_ref, in_v, out_v) = refs[:len(ks)], refs[len(ks):]
    rows, lead = x_refs[0].shape[:2]
    for k, ref in zip(ks, x_refs):
        in_v[pl.ds(pl.multiple_of((me_ref[0] ^ k) * rows, rows), rows)] = ref[...].astype(F32)
    for c in range(lead):
        out_v[:, c, :] = in_v[:, c, :].T
    out_ref[...] = out_v[...].astype(BF16)


def turn_out(me, blocks, lead=8):
    ks = tuple(sorted(blocks))
    rows, chans, seqs = blocks[ks[0]].shape
    res = rows * len(ks)
    return pl.pallas_call(
        functools.partial(turn_out_kernel, ks),
        grid_spec=pltpu.PrefetchScalarGridSpec(
            num_scalar_prefetch=1,
            grid=(seqs // LANES, chans // lead),
            in_specs=[pl.BlockSpec((rows, lead, LANES), lambda k, c, i: (0, c, k)) for _ in ks],
            out_specs=pl.BlockSpec((LANES, lead, res), lambda k, c, i: (k, c, 0)),
            scratch_shapes=[pltpu.VMEM((res, lead, LANES), F32), pltpu.VMEM((LANES, lead, res), F32)],
        ),
        out_shape=jax.ShapeDtypeStruct((seqs, chans, res), BF16),
        cost_estimate=pl.CostEstimate(flops=1 << 24, bytes_accessed=25 << 20, transcendentals=0),
        name='turn_out',
    )(me, *[blocks[k] for k in ks])


def project_kernel(group, idx_ref, *refs):
    count = len(refs) - 12
    x_refs = refs[:count]
    mask_ref, gamma_ref, beta_ref, w_ref, bias_ref, own_ref, sib_ref, b_ref, x_v, a_v, s_in, s_out = refs[count:]
    rows, chans, seqs = x_v.shape[1:]
    hid = b_ref.shape[1]
    half = group * hid
    block = pl.program_id(0)
    slot = lax.rem(block, 2)
    loads = [pltpu.make_async_copy(ref, x_v.at[t], s_in.at[t]) for t, ref in enumerate(x_refs)]
    targets = [own_ref.at[t] for t in range(count // 2)] + [sib_ref.at[t] for t in range(count // 2)]
    saves = [pltpu.make_async_copy(a_v.at[t % 2], target, s_out.at[t % 2]) for t, target in enumerate(targets)]

    @pl.when(block == 0)
    def _():
        for c in loads:
            c.start()

    for t in range(count):
        @pl.when(block == t)
        def _(t=t):
            loads[t].wait()
            if t >= 2:
                saves[t - 2].wait()

    def body(step, carry):
        pieces = []
        for part in range(2):
            first = pl.multiple_of(step * 2 * group + part * group, group)
            x = x_v[block, pl.ds(first, group)].astype(F32)
            centered = x - jnp.mean(x, axis=1, keepdims=True)
            var = jnp.mean(centered * centered, axis=1, keepdims=True)
            y = centered * lax.rsqrt(var + LN_EPS) * gamma_ref[...][None] + beta_ref[...][None]
            y = y.astype(BF16).reshape(group * chans, seqs)
            z = jnp.dot(w_ref[...], y, preferred_element_type=F32) + bias_ref[...]
            mask = mask_ref[pl.ds(first, group), :]
            left = z[:half].reshape(group, hid, seqs) * mask[:, None, :]
            a_v[slot, pl.ds(pl.multiple_of(first * hid, half), half), :] = left.astype(BF16).reshape(half, seqs)
            pieces.append(z[half:].reshape(hid, group, seqs) * mask[None])
        both = jnp.concatenate(pieces, axis=1).astype(BF16)
        b_ref[0, :, pl.ds(pl.multiple_of(step * 2 * group, 2 * group), 2 * group), :] = both
        return carry

    lax.fori_loop(0, rows // (2 * group), body, 0)
    for t in range(count):
        @pl.when(block == t)
        def _(t=t):
            saves[t].start()
            if t == count - 1:
                for c in saves[t - 1:]:
                    c.wait()


def project_weights(w_left, b_left, w_right, b_right, seqs, group=8):
    chans, hid = w_left.shape
    eye = jnp.eye(group, dtype=BF16)
    w_a = jnp.einsum('gh,mp->gphm', eye, w_left).reshape(group * hid, group * chans)
    w_b = jnp.einsum('gh,mq->qghm', eye, w_right).reshape(group * hid, group * chans)
    w_both = jnp.concatenate([w_a, w_b], axis=0)
    bias = jnp.concatenate([jnp.tile(b_left, group), jnp.repeat(b_right, group)]).astype(F32)
    return w_both, jnp.broadcast_to(bias[:, None], (2 * group * hid, seqs))


def project(idx, blocks, mask_t, gamma, beta, w_both, bias, hid, group=8):
    count = len(blocks)
    rows, chans, seqs = blocks[0].shape
    whole = lambda v: pl.BlockSpec(v.shape, lambda s, i: (0,) * v.ndim)
    return pl.pallas_call(
        functools.partial(project_kernel, group),
        grid_spec=pltpu.PrefetchScalarGridSpec(
            num_scalar_prefetch=1,
            grid=(count,),
            in_specs=[ANY] * count + [
                pl.BlockSpec((rows, seqs), lambda s, i: (i[s], 0)),
                whole(gamma), whole(beta), whole(w_both), whole(bias),
            ],
            out_specs=[ANY, ANY, pl.BlockSpec((1, hid, rows, seqs), lambda s, i: (s, 0, 0, 0))],
            scratch_shapes=[
                pltpu.VMEM((count, rows, chans, seqs), BF16),
                pltpu.VMEM((2, rows * hid, seqs), BF16),
                pltpu.SemaphoreType.DMA((count,)),
                pltpu.SemaphoreType.DMA((2,)),
            ],
        ),
        out_shape=[
            jax.ShapeDtypeStruct((count // 2, rows * hid, seqs), BF16),
            jax.ShapeDtypeStruct((count // 2, rows * hid, seqs), BF16),
            jax.ShapeDtypeStruct((count, hid, rows, seqs), BF16),
        ],
        compiler_params=pltpu.CompilerParams(vmem_limit_bytes=48 << 20),
        cost_estimate=pl.CostEstimate(flops=6 << 30, bytes_accessed=13 << 20, transcendentals=0),
        name='project',
    )(idx, *blocks, mask_t, gamma, beta, w_both, bias)


def outer_rows(a, b_v, o_v, qu, ready=None):
    rows, hid, _, cols = o_v.shape

    def q_body(g, carry):
        if ready is not None:
            ready(g)
        for u in range(qu):
            q = g * qu + u
            o = lax.dot_general(a[...], b_v[q], NT, preferred_element_type=F32)
            o_v[:, q] = o.astype(BF16).reshape(rows, hid, cols)
        return carry

    lax.fori_loop(0, hid // qu, q_body, 0)


def weigh_rows(w_ref, o_v, iu, store):
    rows, hid, _, cols = o_v.shape

    def i_body(g, carry):
        for u in range(iu):
            i = g * iu + u
            store(i, jnp.dot(w_ref[...], o_v[i].reshape(hid * hid, cols), preferred_element_type=F32))
        return carry

    lax.fori_loop(0, rows // iu, i_body, 0)


SET_A, SET_B = (0, 2, 4, 1, 3, 5), (6, 7)


def extra_kernel(qu, iu, me_ref, *refs):
    (a_a, a_a_sib, a_b, a_b_sib), b_refs = refs[:4], refs[4:8]
    w_ref, fx, fy, nx, ny, kx, ky, own, a_v, b_v, o_v, r_v, sa, sb, so = refs[8:]
    step = pl.program_id(0)
    slot = lax.rem(step, 2)
    half = kx.shape[0]
    lo, hi = pl.ds(0, half), pl.ds(half, half)
    depth = a_a.shape[2]
    width = b_refs[0].shape[2]

    def a_copies(t):
        pair, at = (((a_b, a_b_sib), 0), ((a_a, a_a_sib), 1), ((a_a, a_a_sib), 2), ((a_a, a_a_sib), 0))[t]
        return [
            pltpu.make_async_copy(ref.at[at], a_v.at[t % 2, :, pl.ds(n * depth, depth)], sa.at[t % 2, n])
            for n, ref in enumerate(pair)
        ]

    def b_copies(g):
        out = []
        qs = pl.ds(g * qu, qu)
        pieces = [(n, ref, t, k) for n, (ref, ks) in enumerate(zip(b_refs, (SET_A, SET_A, SET_B, SET_B))) for t, k in enumerate(ks)]
        for m, (n, ref, t, k) in enumerate(pieces):
            k = k ^ CORE if n % 2 else k
            js = pl.ds(pl.multiple_of((me_ref[0] ^ k) * width, width), width)
            out.append(pltpu.make_async_copy(ref.at[t, qs], b_v.at[qs, js, pl.ds(n % 2 * depth, depth)], sb.at[g, m]))
        return out

    def out_copies(t):
        lower, upper = ((fx, fy), (nx, kx), (ky, ny), (own.at[lo], own.at[hi]))[t]
        sl = t % 2
        return [
            pltpu.make_async_copy(r_v.at[sl, lo], lower, so.at[sl, 0]),
            pltpu.make_async_copy(r_v.at[sl, hi], upper, so.at[sl, 1]),
        ]

    @pl.when(step == 0)
    def _():
        for c in a_copies(0):
            c.start()
        for g in range(b_v.shape[0] // qu):
            for c in b_copies(g):
                c.start()

    for t in range(4):
        @pl.when(step == t)
        def _(t=t):
            for c in a_copies(t):
                c.wait()
            if t < 3:
                for c in a_copies(t + 1):
                    c.start()

    def ready(g):
        @pl.when(step == 0)
        def _():
            for c in b_copies(g):
                c.wait()

    outer_rows(a_v.at[slot], b_v, o_v, qu, ready)
    for t in range(2, 4):
        @pl.when(step == t)
        def _(t=t):
            for c in out_copies(t - 2):
                c.wait()

    def store(i, r):
        r_v[slot, i] = r.astype(BF16)

    weigh_rows(w_ref, o_v, iu, store)
    for t in range(4):
        @pl.when(step == t)
        def _(t=t):
            for c in out_copies(t):
                c.start()
            if t == 3:
                for c in out_copies(2) + out_copies(3):
                    c.wait()


def turn_weights(w_out, hid):
    return w_out.reshape(hid, hid, -1).transpose(2, 1, 0).reshape(-1, hid * hid)


def extra_parts(me, a_parts, b_parts, w_t, cols, qu=8, iu=8):
    hid, depth = b_parts[0].shape[1], 2 * b_parts[0].shape[3]
    rows = a_parts[0].shape[1] // hid
    chans = w_t.shape[0]
    half = rows // 2
    part = lambda *lead: jax.ShapeDtypeStruct(lead + (chans, cols), BF16)
    return pl.pallas_call(
        functools.partial(extra_kernel, qu, iu),
        grid_spec=pltpu.PrefetchScalarGridSpec(
            num_scalar_prefetch=1,
            grid=(4,),
            in_specs=[ANY] * 8 + [pl.BlockSpec(w_t.shape, lambda s, i: (0, 0))],
            out_specs=[ANY] * 7,
            scratch_shapes=[
                pltpu.VMEM((2, rows * hid, depth), BF16),
                pltpu.VMEM((hid, cols, depth), BF16),
                pltpu.VMEM((rows, hid, hid, cols), BF16),
                pltpu.VMEM((2, rows, chans, cols), BF16),
                pltpu.SemaphoreType.DMA((2, 2)),
                pltpu.SemaphoreType.DMA((hid // qu, 16)),
                pltpu.SemaphoreType.DMA((2, 2)),
            ],
        ),
        out_shape=[part(half)] * 6 + [part(rows)],
        compiler_params=pltpu.CompilerParams(vmem_limit_bytes=60 << 20),
        cost_estimate=pl.CostEstimate(flops=60 << 30, bytes_accessed=32 << 20, transcendentals=0),
        name='extra_outer',
    )(me, *a_parts, *b_parts, w_t)


def main_kernel(places, qu, iu, idx_ref, a_ref, *refs):
    b_refs = refs[:len(places)]
    w_ref, bias_ref, inv_ref, z_ref, out_ref, b_v, o_v, sb = refs[len(places):]
    copies = []
    for t, (ref, (k, first)) in enumerate(zip(b_refs, places)):
        count, width = ref.shape[:2]
        at = pl.multiple_of((idx_ref[0] ^ k) * width, width)
        copies.append(pltpu.make_async_copy(ref, b_v.at[pl.ds(first, count), pl.ds(at, width), :], sb.at[t]))
    for c in copies:
        c.start()
    for c in copies:
        c.wait()
    outer_rows(a_ref, b_v, o_v, qu)

    def store(i, r):
        out_ref[i] = z_ref[i] + ((r + bias_ref[...]) * inv_ref[pl.ds(i, 1), :]).T

    weigh_rows(w_ref, o_v, iu, store)


def main_rows(me, a, b_parts, places, w_t, bias, inv, z, qu=8, iu=8):
    hid, _, depth = b_parts[0].shape
    rows, cols, _ = z.shape
    whole = lambda v: pl.BlockSpec(v.shape, lambda s, i: (0,) * v.ndim)
    return pl.pallas_call(
        functools.partial(main_kernel, places, qu, iu),
        grid_spec=pltpu.PrefetchScalarGridSpec(
            num_scalar_prefetch=1,
            grid=(1,),
            in_specs=[whole(a)] + [ANY] * len(b_parts) + [whole(w_t), whole(bias), whole(inv), whole(z)],
            out_specs=whole(z),
            scratch_shapes=[
                pltpu.VMEM((hid, cols, depth), BF16),
                pltpu.VMEM((rows, hid, hid, cols), BF16),
                pltpu.SemaphoreType.DMA((len(b_parts),)),
            ],
        ),
        out_shape=jax.ShapeDtypeStruct(z.shape, F32),
        compiler_params=pltpu.CompilerParams(vmem_limit_bytes=60 << 20),
        cost_estimate=pl.CostEstimate(flops=12 << 30, bytes_accessed=20 << 20, transcendentals=0),
        name='main_outer',
    )(me, a, *b_parts, w_t, bias, inv, z)


def combine_kernel(base_ref, inv_ref, lower_ref, upper_ref, *refs):
    step = pl.program_id(0)
    out_ref = refs[-1]

    def add(ref):
        for i in range(out_ref.shape[0]):
            total = ref[i].astype(F32)
            if len(refs) > 1:
                total = total + refs[0][i].astype(F32) + refs[1][...]
            row = step * out_ref.shape[0] + i
            out_ref[i] = base_ref[i] + (total * inv_ref[pl.ds(row, 1), :]).T

    @pl.when(step < pl.num_programs(0) // 2)
    def _():
        add(lower_ref)

    @pl.when(step >= pl.num_programs(0) // 2)
    def _():
        add(upper_ref)


def combine(base, inv, lower, upper, own=None, bias=None, block=16):
    rows, cols, chans = base.shape
    mid = rows // block // 2
    flat = lambda: pl.BlockSpec((block, cols, chans), lambda s: (s, 0, 0))
    extra, extra_specs = (), []
    if own is not None:
        extra = (own, bias)
        extra_specs = [pl.BlockSpec((block, chans, cols), lambda s: (s, 0, 0)), pl.BlockSpec((chans, cols), lambda s: (0, 0))]
    return pl.pallas_call(
        combine_kernel,
        grid=(2 * mid,),
        in_specs=[
            flat(),
            pl.BlockSpec((rows, cols), lambda s: (0, 0)),
            pl.BlockSpec((block, chans, cols), lambda s: (jnp.minimum(s, mid - 1), 0, 0)),
            pl.BlockSpec((block, chans, cols), lambda s: (jnp.maximum(s - mid, 0), 0, 0)),
        ] + extra_specs,
        out_specs=flat(),
        out_shape=jax.ShapeDtypeStruct(base.shape, F32),
        compiler_params=pltpu.CompilerParams(vmem_limit_bytes=24 << 20),
        cost_estimate=pl.CostEstimate(flops=1 << 24, bytes_accessed=15 << 20, transcendentals=0),
        name='combine',
    )(base, inv, lower, upper, *extra)


def assemble_kernel(ref, out_ref):
    width = ref.shape[2]
    for d in range(ref.shape[0]):
        out_ref[:, d * width:(d + 1) * width, :] = ref[d]


def assemble(value, block=8):
    srcs, seqs, width, chans = value.shape
    return pl.pallas_call(
        assemble_kernel,
        grid=(seqs // block,),
        in_specs=[pl.BlockSpec((srcs, block, width, chans), lambda s: (0, s, 0, 0))],
        out_specs=pl.BlockSpec((block, srcs * width, chans), lambda s: (s, 0, 0)),
        out_shape=jax.ShapeDtypeStruct((seqs, srcs * width, chans), value.dtype),
        cost_estimate=pl.CostEstimate(flops=1 << 24, bytes_accessed=16 << 20, transcendentals=0),
        name='assemble',
    )(value)


def layer_norm(value, gamma, beta):
    as_float = value.astype(F32)
    mean = jnp.mean(as_float, axis=-1, keepdims=True)
    centered = as_float - mean
    var = jnp.mean(centered * centered, axis=-1, keepdims=True)
    return (centered * lax.rsqrt(var + LN_EPS) * gamma.astype(F32) + beta.astype(F32)).astype(BF16)


def inverse_norms(mask, mask_rows):
    counts = jnp.einsum('si,sj->ij', mask_rows.astype(BF16), mask.astype(BF16), preferred_element_type=F32)
    return 1.0 / (NORM_EPS + counts)


def solution(mesh):
    size = mesh.shape['dap']
    value_spec = P('data', 'dap', None)
    mask_spec = P('data', None)
    row_spec = P(('data', 'dap'), None, None)

    def local_program(extra_block, extra_mask, main_block, main_mask, pair_rows, eg, eb, ewl, ebl, ewr, ebr, ewo, ebo, mg, mb, mwl, mbl, mwr, mbr, mwo, mbo):
        me = lax.axis_index('dap')
        rows = extra_block.shape[1]
        hid = ewl.shape[1]

        seqs = extra_block.shape[0] // size
        cols = size * rows
        minor = extra_block.transpose(1, 2, 0)
        me1 = me.astype(jnp.int32)[None]
        turned = dict(zip(NEAR[:2], turn(me1, minor, NEAR[:2], size)))
        turned.update(zip(NEAR[2:], turn(me1, minor, NEAR[2:], size)))
        turned.update(zip(REST, turn(me1, minor, REST, size)))
        blocks = {0: turned[0]}
        for k in NEAR[:2]:
            blocks[k] = swap(turned[k], k, size)
        for k in NEAR[2:]:
            blocks[k] = swap(turned[k], k, size)
        blocks[1] = swap(turned[1], CORE, size)
        near, far = lax.optimization_barrier(([blocks[k] for k in NEAR[:2]], [turned[6], turned[7]]))
        blocks.update(zip(NEAR[:2], near))
        for k, value in zip((6, 7), far):
            blocks[k] = swap(value, k, size)

        mask_rows_m = lax.dynamic_slice_in_dim(main_mask, me * rows, rows, axis=1)
        mask_rows_e = lax.dynamic_slice_in_dim(extra_mask, me * rows, rows, axis=1)
        inv_m = inverse_norms(main_mask, mask_rows_m)
        inv_e = inverse_norms(extra_mask, mask_rows_e)
        normed = layer_norm(main_block, mg, mb)
        mask_m = mask_rows_m.astype(F32).T
        a_m = jnp.einsum('sim,mp->ips', normed, mwl, preferred_element_type=F32) + mbl.astype(F32)[None, :, None]
        a_m = (a_m * mask_m[:, None, :]).astype(BF16).reshape(rows * hid, -1)
        b_m = jnp.einsum('sim,mq->qis', normed, mwr, preferred_element_type=F32) + mbr.astype(F32)[:, None, None]
        b_m = (b_m * mask_m[None]).astype(BF16)

        wide = lambda v, n: jnp.broadcast_to(v.astype(F32)[:, None], (v.shape[0], n))
        mask_seq = lax.dynamic_slice_in_dim(extra_mask, me * seqs, seqs, axis=0).astype(F32).T
        w_both, bias = project_weights(ewl, ebl, ewr, ebr, seqs)
        gamma, beta = wide(eg, seqs), wide(eb, seqs)
        idx_a, idx_b = [(me ^ jnp.array(ks, jnp.int32)).astype(jnp.int32) for ks in (SET_A, SET_B)]
        w_e, w_m = turn_weights(ewo, hid), turn_weights(mwo, hid)
        bias_e, bias_m = wide(ebo, cols), wide(mbo, cols)

        a_a, a_a_give, b_a = project(idx_a, [blocks[k] for k in SET_A], mask_seq, gamma, beta, w_both, bias, hid)
        a_a_sib, b_a_sib = swap(a_a_give, CORE, size), swap(b_a, CORE, size)

        blocks[6], blocks[7], main_moved = lax.optimization_barrier((blocks[6], blocks[7], main_block))
        main_moved = lax.all_to_all(main_moved, 'dap', 0, 0, tiled=True).reshape(size, -1, rows, main_block.shape[2])
        b_x, b_y = swap(b_m, XBIT, size), swap(b_m, YBIT, size)
        mid = hid // 2
        b_d = [swap(b_x[:mid], YBIT, size), swap(b_y[mid:], XBIT, size)]
        b_parts = [b_m, b_x, b_y]
        b_parts = b_parts + [swap(part, CORE, size) for part in b_parts]
        b_parts = b_parts + b_d + [swap(part, CORE, size) for part in b_d]
        places = ((0, 0), (XBIT, 0), (YBIT, 0), (CORE, 0), (CORE | XBIT, 0), (CORE | YBIT, 0))
        places = places + ((XBIT | YBIT, 0), (XBIT | YBIT, mid), (CORE | XBIT | YBIT, 0), (CORE | XBIT | YBIT, mid))

        a_b, a_b_give, b_b = project(idx_b, [blocks[k] for k in SET_B], mask_seq, gamma, beta, w_both, bias, hid)
        a_b_sib, b_b_sib = swap(a_b_give, CORE, size), swap(b_b, CORE, size)
        fx, fy, nx, ny, kx, ky, own = extra_parts(me1, (a_a, a_a_sib, a_b, a_b_sib), (b_a, b_a_sib, b_b, b_b_sib), w_e, cols)
        fx, fy = swap(fx, XBIT, size), swap(fy, YBIT, size)
        nx, ny = swap(nx, XBIT, size), swap(ny, YBIT, size)
        kx = (kx.astype(F32) + fy.astype(F32)).astype(BF16)
        ky = (ky.astype(F32) + fx.astype(F32)).astype(BF16)
        kx, ky = swap(kx, XBIT, size), swap(ky, YBIT, size)

        base = main_rows(me1, a_m, b_parts, places, w_m, bias_m, inv_m, pair_rows)
        main_out = assemble(main_moved)
        extra_out = turn_out(me1, blocks).transpose(0, 2, 1)
        base = combine(base, inv_e, nx, ny, own, bias_e)
        pair_out = combine(base, inv_e, ky, kx)
        return pair_out, extra_out, main_out

    in_specs = (value_spec, mask_spec, value_spec, mask_spec, row_spec) + (P(),) * 16
    return jax.shard_map(local_program, mesh=mesh, in_specs=in_specs, out_specs=(row_spec, row_spec, row_spec), check_vma=False)
```

```python
import functools

import jax
import jax.numpy as jnp
from jax import lax
from jax.experimental import pallas as pl
from jax.experimental.pallas import tpu as pltpu
from jax.sharding import PartitionSpec as P


LN_EPS = 1e-5
NORM_EPS = 1e-3
NT = (((1,), (1,)), ((), ()))
F32 = jnp.float32
BF16 = jnp.bfloat16
ANY = pl.BlockSpec(memory_space=pl.ANY)
CORE, XBIT, YBIT = 1, 2, 4
LANES = 128
NEAR, REST = (2, 4, 3, 5), (6, 7, 1, 0)


def swap(value, bit, size):
    return lax.ppermute(value, 'dap', [(d, d ^ bit) for d in range(size)])


def turn_kernel(ks, me_ref, x_ref, *refs):
    outs, (v, s_in, s_out) = refs[:len(ks)], refs[len(ks):]
    seqs = v.shape[3]
    loads = [
        pltpu.make_async_copy(x_ref.at[:, :, pl.ds(pl.multiple_of((me_ref[0] ^ k) * seqs, LANES), seqs)], v.at[t], s_in.at[t])
        for t, k in enumerate(ks)
    ]
    stores = [pltpu.make_async_copy(v.at[t], out, s_out.at[t]) for t, out in enumerate(outs)]
    for c in loads:
        c.start()
    for load, save in zip(loads, stores):
        load.wait()
        save.start()
    for c in stores:
        c.wait()


def turn(me, x, ks, size):
    rows, chans, total = x.shape
    seqs = total // size
    return pl.pallas_call(
        functools.partial(turn_kernel, ks),
        grid_spec=pltpu.PrefetchScalarGridSpec(
            num_scalar_prefetch=1,
            grid=(1,),
            in_specs=[ANY],
            out_specs=[ANY] * len(ks),
            scratch_shapes=[
                pltpu.VMEM((len(ks), rows, chans, seqs), x.dtype),
                pltpu.SemaphoreType.DMA((len(ks),)),
                pltpu.SemaphoreType.DMA((len(ks),)),
            ],
        ),
        out_shape=[jax.ShapeDtypeStruct((rows, chans, seqs), x.dtype) for _ in ks],
        cost_estimate=pl.CostEstimate(flops=1 << 24, bytes_accessed=4 << 20, transcendentals=0),
        name='turn',
    )(me, x)


def turn_out_kernel(ks, me_ref, *refs):
    x_refs, (out_ref, in_v, out_v) = refs[:len(ks)], refs[-3:]
    rows, lead = x_refs[0].shape[:2]
    for k, ref in zip(ks, x_refs):
        at = lax.rem(me_ref[0] ^ k, len(ks)) * rows
        in_v[pl.ds(pl.multiple_of(at, rows), rows)] = ref[...].astype(F32)
    for c in range(lead):
        out_v[:, c, :] = in_v[:, c, :].T
    out_ref[...] = out_v[...].astype(BF16)


def turn_out(me, blocks, ks, size, into=None, lead=16):
    rows, chans, seqs = blocks[ks[0]].shape
    res = rows * len(ks)
    halves = size // len(ks)
    carried = [] if into is None else [into]
    return pl.pallas_call(
        functools.partial(turn_out_kernel, ks),
        grid_spec=pltpu.PrefetchScalarGridSpec(
            num_scalar_prefetch=1,
            grid=(seqs // LANES, chans // lead),
            in_specs=[pl.BlockSpec((rows, lead, LANES), lambda k, c, i: (0, c, k)) for _ in ks] + [ANY] * len(carried),
            out_specs=pl.BlockSpec((LANES, lead, res), lambda k, c, i: (k, c, (i[0] ^ ks[0]) // len(ks))),
            scratch_shapes=[pltpu.VMEM((res, lead, LANES), F32), pltpu.VMEM((LANES, lead, res), F32)],
        ),
        out_shape=jax.ShapeDtypeStruct((seqs, chans, halves * res), BF16),
        input_output_aliases={len(ks) + 1: 0} if carried else {},
        cost_estimate=pl.CostEstimate(flops=1 << 24, bytes_accessed=13 << 20, transcendentals=0),
        name='turn_out',
    )(me, *[blocks[k] for k in ks], *carried)


def project_kernel(group, idx_ref, *refs):
    count = len(refs) - 12
    x_refs = refs[:count]
    mask_ref, gamma_ref, beta_ref, w_ref, bias_ref, own_ref, sib_ref, b_ref, x_v, a_v, s_in, s_out = refs[count:]
    rows, chans, seqs = x_v.shape[1:]
    hid = b_ref.shape[1]
    half = group * hid
    block = pl.program_id(0)
    slot = lax.rem(block, 2)
    loads = [pltpu.make_async_copy(ref, x_v.at[t], s_in.at[t]) for t, ref in enumerate(x_refs)]
    targets = [own_ref.at[t] for t in range(count // 2)] + [sib_ref.at[t] for t in range(count // 2)]
    saves = [pltpu.make_async_copy(a_v.at[t % 2], target, s_out.at[t % 2]) for t, target in enumerate(targets)]

    @pl.when(block == 0)
    def _():
        for c in loads:
            c.start()

    for t in range(count):
        @pl.when(block == t)
        def _(t=t):
            loads[t].wait()
            if t >= 2:
                saves[t - 2].wait()

    def body(step, carry):
        pieces = []
        for part in range(2):
            first = pl.multiple_of(step * 2 * group + part * group, group)
            x = x_v[block, pl.ds(first, group)].astype(F32)
            centered = x - jnp.mean(x, axis=1, keepdims=True)
            var = jnp.mean(centered * centered, axis=1, keepdims=True)
            y = centered * lax.rsqrt(var + LN_EPS) * gamma_ref[...][None] + beta_ref[...][None]
            y = y.astype(BF16).reshape(group * chans, seqs)
            z = jnp.dot(w_ref[...], y, preferred_element_type=F32) + bias_ref[...]
            mask = mask_ref[pl.ds(first, group), :]
            left = z[:half].reshape(group, hid, seqs) * mask[:, None, :]
            a_v[slot, pl.ds(pl.multiple_of(first * hid, half), half), :] = left.astype(BF16).reshape(half, seqs)
            pieces.append(z[half:].reshape(hid, group, seqs) * mask[None])
        both = jnp.concatenate(pieces, axis=1).astype(BF16)
        b_ref[0, :, pl.ds(pl.multiple_of(step * 2 * group, 2 * group), 2 * group), :] = both
        return carry

    lax.fori_loop(0, rows // (2 * group), body, 0)
    for t in range(count):
        @pl.when(block == t)
        def _(t=t):
            saves[t].start()
            if t == count - 1:
                for c in saves[t - 1:]:
                    c.wait()


def project_weights(w_left, b_left, w_right, b_right, seqs, group=8):
    chans, hid = w_left.shape
    eye = jnp.eye(group, dtype=BF16)
    w_a = jnp.einsum('gh,mp->gphm', eye, w_left).reshape(group * hid, group * chans)
    w_b = jnp.einsum('gh,mq->qghm', eye, w_right).reshape(group * hid, group * chans)
    w_both = jnp.concatenate([w_a, w_b], axis=0)
    bias = jnp.concatenate([jnp.tile(b_left, group), jnp.repeat(b_right, group)]).astype(F32)
    return w_both, jnp.broadcast_to(bias[:, None], (2 * group * hid, seqs))


def project(idx, blocks, mask_t, gamma, beta, w_both, bias, hid, group=8):
    count = len(blocks)
    rows, chans, seqs = blocks[0].shape
    whole = lambda v: pl.BlockSpec(v.shape, lambda s, i: (0,) * v.ndim)
    return pl.pallas_call(
        functools.partial(project_kernel, group),
        grid_spec=pltpu.PrefetchScalarGridSpec(
            num_scalar_prefetch=1,
            grid=(count,),
            in_specs=[ANY] * count + [
                pl.BlockSpec((rows, seqs), lambda s, i: (i[s], 0)),
                whole(gamma), whole(beta), whole(w_both), whole(bias),
            ],
            out_specs=[ANY, ANY, pl.BlockSpec((1, hid, rows, seqs), lambda s, i: (s, 0, 0, 0))],
            scratch_shapes=[
                pltpu.VMEM((count, rows, chans, seqs), BF16),
                pltpu.VMEM((2, rows * hid, seqs), BF16),
                pltpu.SemaphoreType.DMA((count,)),
                pltpu.SemaphoreType.DMA((2,)),
            ],
        ),
        out_shape=[
            jax.ShapeDtypeStruct((count // 2, rows * hid, seqs), BF16),
            jax.ShapeDtypeStruct((count // 2, rows * hid, seqs), BF16),
            jax.ShapeDtypeStruct((count, hid, rows, seqs), BF16),
        ],
        compiler_params=pltpu.CompilerParams(vmem_limit_bytes=48 << 20),
        cost_estimate=pl.CostEstimate(flops=6 << 30, bytes_accessed=13 << 20, transcendentals=0),
        name='project',
    )(idx, *blocks, mask_t, gamma, beta, w_both, bias)


def outer_rows(a, b_v, o_v, qu, ready=None, more=None):
    rows, hid, _, cols = o_v.shape

    def q_body(g, carry):
        if ready is not None:
            ready(g)
        for u in range(qu):
            q = g * qu + u
            o = lax.dot_general(a[...], b_v[q], NT, preferred_element_type=F32)
            if more is not None:
                o = o + jnp.dot(more[0][...], more[1][q], preferred_element_type=F32)
            o_v[:, q] = o.astype(BF16).reshape(rows, hid, cols)
        return carry

    lax.fori_loop(0, hid // qu, q_body, 0)


def weigh_rows(w_ref, o_v, iu, store):
    rows, hid, _, cols = o_v.shape

    def i_body(g, carry):
        for u in range(iu):
            i = g * iu + u
            store(i, jnp.dot(w_ref[...], o_v[i].reshape(hid * hid, cols), preferred_element_type=F32))
        return carry

    lax.fori_loop(0, rows // iu, i_body, 0)


SET_A, SET_B = (0, 2, 4, 1, 3, 5), (6, 7)


def extra_kernel(qu, iu, me_ref, *refs):
    (a_a, a_a_sib, a_b, a_b_sib), b_refs = refs[:4], refs[4:8]
    w_ref, fx, fy, nx, ny, kx, ky, own, a_v, b_v, o_v, r_v, sa, sb, so = refs[8:]
    step = pl.program_id(0)
    slot = lax.rem(step, 2)
    half = kx.shape[0]
    lo, hi = pl.ds(0, half), pl.ds(half, half)
    depth = a_a.shape[2]
    width = b_refs[0].shape[2]

    def a_copies(t):
        pair, at = (((a_b, a_b_sib), 0), ((a_a, a_a_sib), 1), ((a_a, a_a_sib), 2), ((a_a, a_a_sib), 0))[t]
        return [
            pltpu.make_async_copy(ref.at[at], a_v.at[t % 2, :, pl.ds(n * depth, depth)], sa.at[t % 2, n])
            for n, ref in enumerate(pair)
        ]

    def b_copies(g):
        out = []
        qs = pl.ds(g * qu, qu)
        pieces = [(n, ref, t, k) for n, (ref, ks) in enumerate(zip(b_refs, (SET_A, SET_A, SET_B, SET_B))) for t, k in enumerate(ks)]
        for m, (n, ref, t, k) in enumerate(pieces):
            k = k ^ CORE if n % 2 else k
            js = pl.ds(pl.multiple_of((me_ref[0] ^ k) * width, width), width)
            out.append(pltpu.make_async_copy(ref.at[t, qs], b_v.at[qs, js, pl.ds(n % 2 * depth, depth)], sb.at[g, m]))
        return out

    def out_copies(t):
        lower, upper = ((fx, fy), (nx, kx), (ky, ny), (own.at[lo], own.at[hi]))[t]
        sl = t % 2
        return [
            pltpu.make_async_copy(r_v.at[sl, lo], lower, so.at[sl, 0]),
            pltpu.make_async_copy(r_v.at[sl, hi], upper, so.at[sl, 1]),
        ]

    @pl.when(step == 0)
    def _():
        for c in a_copies(0):
            c.start()
        for g in range(b_v.shape[0] // qu):
            for c in b_copies(g):
                c.start()

    for t in range(4):
        @pl.when(step == t)
        def _(t=t):
            for c in a_copies(t):
                c.wait()
            if t < 3:
                for c in a_copies(t + 1):
                    c.start()

    def ready(g):
        @pl.when(step == 0)
        def _():
            for c in b_copies(g):
                c.wait()

    outer_rows(a_v.at[slot], b_v, o_v, qu, ready)
    for t in range(2, 4):
        @pl.when(step == t)
        def _(t=t):
            for c in out_copies(t - 2):
                c.wait()

    def store(i, r):
        r_v[slot, i] = r.astype(BF16)

    weigh_rows(w_ref, o_v, iu, store)
    for t in range(4):
        @pl.when(step == t)
        def _(t=t):
            for c in out_copies(t):
                c.start()
            if t == 3:
                for c in out_copies(2) + out_copies(3):
                    c.wait()


def turn_weights(w_out, hid):
    return w_out.reshape(hid, hid, -1).transpose(2, 1, 0).reshape(-1, hid * hid)


def extra_parts(me, a_parts, b_parts, w_t, cols, qu=8, iu=8):
    hid, depth = b_parts[0].shape[1], 2 * b_parts[0].shape[3]
    rows = a_parts[0].shape[1] // hid
    chans = w_t.shape[0]
    half = rows // 2
    part = lambda *lead: jax.ShapeDtypeStruct(lead + (chans, cols), BF16)
    return pl.pallas_call(
        functools.partial(extra_kernel, qu, iu),
        grid_spec=pltpu.PrefetchScalarGridSpec(
            num_scalar_prefetch=1,
            grid=(4,),
            in_specs=[ANY] * 8 + [pl.BlockSpec(w_t.shape, lambda s, i: (0, 0))],
            out_specs=[ANY] * 7,
            scratch_shapes=[
                pltpu.VMEM((2, rows * hid, depth), BF16),
                pltpu.VMEM((hid, cols, depth), BF16),
                pltpu.VMEM((rows, hid, hid, cols), BF16),
                pltpu.VMEM((2, rows, chans, cols), BF16),
                pltpu.SemaphoreType.DMA((2, 2)),
                pltpu.SemaphoreType.DMA((hid // qu, 16)),
                pltpu.SemaphoreType.DMA((2, 2)),
            ],
        ),
        out_shape=[part(half)] * 6 + [part(rows)],
        compiler_params=pltpu.CompilerParams(vmem_limit_bytes=60 << 20),
        cost_estimate=pl.CostEstimate(flops=60 << 30, bytes_accessed=32 << 20, transcendentals=0),
        name='extra_outer',
    )(me, *a_parts, *b_parts, w_t)


def main_late_kernel(x_ref, mask_ref, gamma_ref, beta_ref, w_ref, bias_ref, out_ref, z_v):
    srcs, seqs, rows, chans = x_ref.shape
    hid = w_ref.shape[0]

    def body(g, carry):
        for u in range(4):
            n = g * 4 + u
            x = x_ref[:, n].reshape(srcs * rows, chans).astype(F32)
            centered = x - jnp.mean(x, axis=1, keepdims=True)
            var = jnp.mean(centered * centered, axis=1, keepdims=True)
            y = (centered * lax.rsqrt(var + LN_EPS) * gamma_ref[...] + beta_ref[...]).astype(BF16)
            z = lax.dot_general(w_ref[...], y, NT, preferred_element_type=F32) + bias_ref[...]
            z_v[n] = z * mask_ref[pl.ds(n, 1), :]
        return carry

    lax.fori_loop(0, seqs // 4, body, 0)
    for q in range(hid):
        out_ref[q] = z_v[:, q, :].astype(BF16)


def main_late(moved, mask, gamma, beta, w_right, b_right, block=16):
    srcs, seqs, rows, chans = moved.shape
    hid = w_right.shape[1]
    res = srcs * rows
    whole = lambda v: pl.BlockSpec(v.shape, lambda s: (0,) * v.ndim)
    row = lambda v: v.astype(F32)[None]
    bias = jnp.broadcast_to(b_right.astype(F32)[:, None], (hid, res))
    args = (row(gamma), row(beta), w_right.T, bias)
    return pl.pallas_call(
        main_late_kernel,
        grid=(seqs // block,),
        in_specs=[
            pl.BlockSpec((srcs, block, rows, chans), lambda s: (0, s, 0, 0)),
            pl.BlockSpec((block, res), lambda s: (s, 0)),
        ] + [whole(v) for v in args],
        out_specs=pl.BlockSpec((hid, block, res), lambda s: (0, s, 0)),
        out_shape=jax.ShapeDtypeStruct((hid, seqs, res), BF16),
        scratch_shapes=[pltpu.VMEM((block, hid, res), F32)],
        compiler_params=pltpu.CompilerParams(vmem_limit_bytes=32 << 20),
        cost_estimate=pl.CostEstimate(flops=4 << 30, bytes_accessed=10 << 20, transcendentals=0),
        name='main_late',
    )(moved, mask, *args)


HID = 32
OWN_X = ((0, HID, 0, 0, 3), (HID, HID, 0, 0, 2))
OWN_Y = ((HID, HID, 0, 0, 1),)
FROM_X = ((0, HID, XBIT, 0, 2), (HID, HID, XBIT, 0, 3), (2 * HID, HID, XBIT, 0, 1))
FROM_Y = ((0, HID, YBIT, 0, 2), (HID, HID, YBIT, 0, 3), (2 * HID, HID, YBIT, 0, 1))
FAR_Y = ((0, HID, XBIT | YBIT, 0, 1), (HID, HID // 2, XBIT | YBIT, 0, 3))
FAR_X = ((0, HID // 2, XBIT | YBIT, HID // 2, 3), (HID // 2, HID, XBIT | YBIT, 0, 2))


def main_kernel(tables, qu, iu, idx_ref, a_ref, *refs):
    b_refs, late_refs = refs[:len(tables)], refs[len(tables):len(tables) + 2]
    w_ref, bias_ref, inv_ref, z_ref, out_ref, a_v, c_v, b_v, l_v, o_v, sa, sb = refs[len(tables) + 2:]
    me = idx_ref[0]
    chip, core = me // 2, lax.rem(me, 2)
    copies = []
    lanes = lambda n: pl.ds(pl.multiple_of(n * LANES, LANES), LANES)
    for r in range(4):
        target = c_v if r == 0 else a_v.at[:, lanes(r - 1)]
        copies.append(pltpu.make_async_copy(a_ref.at[:, lanes(chip ^ r)], target, sa.at[r]))
    for n, ref in enumerate(late_refs):
        seqs = ref.shape[1]
        at = pl.ds(pl.multiple_of((core ^ n) * seqs, seqs), seqs)
        copies.append(pltpu.make_async_copy(ref, l_v.at[:, at, :], sa.at[4 + n]))
    count = 0
    for ref, (core_bit, table) in zip(b_refs, tables):
        for first, rows, k, q, r in table:
            width = ref.shape[1]
            js = pl.ds(pl.multiple_of((me ^ k ^ core_bit) * width, width), width)
            copies.append(pltpu.make_async_copy(ref.at[pl.ds(first, rows)], b_v.at[pl.ds(q, rows), js, lanes(r - 1)], sb.at[count]))
            count += 1
    for c in copies:
        c.start()
    for c in copies:
        c.wait()
    outer_rows(a_v, b_v, o_v, qu, more=(c_v, l_v))

    def store(i, r):
        out_ref[i] = z_ref[i] + ((r + bias_ref[...]) * inv_ref[pl.ds(i, 1), :]).T

    weigh_rows(w_ref, o_v, iu, store)


def main_rows(me, a, b_parts, tables, late, w_t, bias, inv, z, qu=8, iu=8):
    rows, cols, _ = z.shape
    hid = a.shape[0] // rows
    count = sum(len(table) for _, table in tables)
    whole = lambda v: pl.BlockSpec(v.shape, lambda s, i: (0,) * v.ndim)
    return pl.pallas_call(
        functools.partial(main_kernel, tables, qu, iu),
        grid_spec=pltpu.PrefetchScalarGridSpec(
            num_scalar_prefetch=1,
            grid=(1,),
            in_specs=[ANY] * (len(b_parts) + 3) + [whole(w_t), whole(bias), whole(inv), whole(z)],
            out_specs=whole(z),
            scratch_shapes=[
                pltpu.VMEM((rows * hid, 3 * LANES), BF16),
                pltpu.VMEM((rows * hid, LANES), BF16),
                pltpu.VMEM((hid, cols, 3 * LANES), BF16),
                pltpu.VMEM((hid, LANES, cols), BF16),
                pltpu.VMEM((rows, hid, hid, cols), BF16),
                pltpu.SemaphoreType.DMA((6,)),
                pltpu.SemaphoreType.DMA((count,)),
            ],
        ),
        out_shape=jax.ShapeDtypeStruct(z.shape, F32),
        compiler_params=pltpu.CompilerParams(vmem_limit_bytes=60 << 20),
        cost_estimate=pl.CostEstimate(flops=12 << 30, bytes_accessed=20 << 20, transcendentals=0),
        name='main_outer',
    )(me, a, *b_parts, *late, w_t, bias, inv, z)


def combine_kernel(base_ref, inv_ref, lower_ref, upper_ref, *refs):
    step = pl.program_id(0)
    out_ref = refs[-1]

    def add(ref):
        for i in range(out_ref.shape[0]):
            total = ref[i].astype(F32)
            if len(refs) > 1:
                total = total + refs[0][i].astype(F32) + refs[1][...]
            row = step * out_ref.shape[0] + i
            out_ref[i] = base_ref[i] + (total * inv_ref[pl.ds(row, 1), :]).T

    @pl.when(step < pl.num_programs(0) // 2)
    def _():
        add(lower_ref)

    @pl.when(step >= pl.num_programs(0) // 2)
    def _():
        add(upper_ref)


def combine(base, inv, lower, upper, own=None, bias=None, block=16):
    rows, cols, chans = base.shape
    mid = rows // block // 2
    flat = lambda: pl.BlockSpec((block, cols, chans), lambda s: (s, 0, 0))
    extra, extra_specs = (), []
    if own is not None:
        extra = (own, bias)
        extra_specs = [pl.BlockSpec((block, chans, cols), lambda s: (s, 0, 0)), pl.BlockSpec((chans, cols), lambda s: (0, 0))]
    return pl.pallas_call(
        combine_kernel,
        grid=(2 * mid,),
        in_specs=[
            flat(),
            pl.BlockSpec((rows, cols), lambda s: (0, 0)),
            pl.BlockSpec((block, chans, cols), lambda s: (jnp.minimum(s, mid - 1), 0, 0)),
            pl.BlockSpec((block, chans, cols), lambda s: (jnp.maximum(s - mid, 0), 0, 0)),
        ] + extra_specs,
        out_specs=flat(),
        out_shape=jax.ShapeDtypeStruct(base.shape, F32),
        compiler_params=pltpu.CompilerParams(vmem_limit_bytes=24 << 20),
        cost_estimate=pl.CostEstimate(flops=1 << 24, bytes_accessed=15 << 20, transcendentals=0),
        name='combine',
    )(base, inv, lower, upper, *extra)


def assemble_kernel(ref, out_ref):
    width = ref.shape[2]
    for d in range(ref.shape[0]):
        out_ref[:, d * width:(d + 1) * width, :] = ref[d]


def assemble(value, block=8):
    srcs, seqs, width, chans = value.shape
    return pl.pallas_call(
        assemble_kernel,
        grid=(seqs // block,),
        in_specs=[pl.BlockSpec((srcs, block, width, chans), lambda s: (0, s, 0, 0))],
        out_specs=pl.BlockSpec((block, srcs * width, chans), lambda s: (s, 0, 0)),
        out_shape=jax.ShapeDtypeStruct((seqs, srcs * width, chans), value.dtype),
        cost_estimate=pl.CostEstimate(flops=1 << 24, bytes_accessed=16 << 20, transcendentals=0),
        name='assemble',
    )(value)


def layer_norm(value, gamma, beta):
    as_float = value.astype(F32)
    mean = jnp.mean(as_float, axis=-1, keepdims=True)
    centered = as_float - mean
    var = jnp.mean(centered * centered, axis=-1, keepdims=True)
    return (centered * lax.rsqrt(var + LN_EPS) * gamma.astype(F32) + beta.astype(F32)).astype(BF16)


def inverse_norms(mask, mask_rows):
    counts = jnp.einsum('si,sj->ij', mask_rows.astype(BF16), mask.astype(BF16), preferred_element_type=F32)
    return 1.0 / (NORM_EPS + counts)


def solution(mesh):
    size = mesh.shape['dap']
    value_spec = P('data', 'dap', None)
    mask_spec = P('data', None)
    row_spec = P(('data', 'dap'), None, None)

    def local_program(extra_block, extra_mask, main_block, main_mask, pair_rows, eg, eb, ewl, ebl, ewr, ebr, ewo, ebo, mg, mb, mwl, mbl, mwr, mbr, mwo, mbo):
        me = lax.axis_index('dap')
        chip = me // 2
        rows = extra_block.shape[1]
        hid = ewl.shape[1]

        seqs = extra_block.shape[0] // size
        cols = size * rows
        minor = extra_block.transpose(1, 2, 0)
        me1 = me.astype(jnp.int32)[None]
        turned = dict(zip(NEAR[:2], turn(me1, minor, NEAR[:2], size)))
        turned.update(zip(NEAR[2:], turn(me1, minor, NEAR[2:], size)))
        turned.update(zip(REST, turn(me1, minor, REST, size)))
        blocks = {0: turned[0]}
        for k in NEAR[:2]:
            blocks[k] = swap(turned[k], k, size)
        for k in NEAR[2:]:
            blocks[k] = swap(turned[k], k, size)
        blocks[1] = swap(turned[1], CORE, size)
        near, far = lax.optimization_barrier(([blocks[k] for k in NEAR], [turned[6], turned[7]]))
        blocks.update(zip(NEAR, near))
        for k, value in zip((6, 7), far):
            blocks[k] = swap(value, k, size)

        mask_rows_m = lax.dynamic_slice_in_dim(main_mask, me * rows, rows, axis=1)
        normed = layer_norm(main_block, mg, mb)
        mask_m = mask_rows_m.astype(F32).T

        wide = lambda v, n: jnp.broadcast_to(v.astype(F32)[:, None], (v.shape[0], n))
        mask_seq = lax.dynamic_slice_in_dim(extra_mask, me * seqs, seqs, axis=0).astype(F32).T
        w_both, bias = project_weights(ewl, ebl, ewr, ebr, seqs)
        gamma, beta = wide(eg, seqs), wide(eb, seqs)
        idx_a, idx_b = [(me ^ jnp.array(ks, jnp.int32)).astype(jnp.int32) for ks in (SET_A, SET_B)]
        a_m = jnp.einsum('sim,mp->ips', normed, mwl, preferred_element_type=F32) + mbl.astype(F32)[None, :, None]
        a_m = (a_m * mask_m[:, None, :]).astype(BF16).reshape(rows * hid, -1)
        b_m = jnp.einsum('sim,mq->qis', normed, mwr, preferred_element_type=F32) + mbr.astype(F32)[:, None, None]
        b_m = (b_m * mask_m[None]).astype(BF16)
        pick = lambda r: lax.dynamic_slice_in_dim(b_m, (chip ^ r) * LANES, LANES, axis=2)
        b_0, b_1, b_2, b_3 = [pick(r) for r in range(4)]
        b_to_x, b_to_y = jnp.concatenate([b_3, b_2, b_0]), jnp.concatenate([b_0, b_1, b_3])
        mask_rows_e = lax.dynamic_slice_in_dim(extra_mask, me * rows, rows, axis=1)
        inv_m = inverse_norms(main_mask, mask_rows_m)
        inv_e = inverse_norms(extra_mask, mask_rows_e)
        w_e, w_m = turn_weights(ewo, hid), turn_weights(mwo, hid)
        bias_e, bias_m = wide(ebo, cols), wide(mbo, cols)
        count = main_mask.shape[0] // size
        mask_late = lax.dynamic_slice_in_dim(main_mask, me * count, count, axis=0).astype(F32)

        a_a, a_a_give, b_a = project(idx_a, [blocks[k] for k in SET_A], mask_seq, gamma, beta, w_both, bias, hid)
        a_a_sib, b_a_sib = swap(a_a_give, CORE, size), swap(b_a, CORE, size)

        blocks[6], blocks[7], main_moved = lax.optimization_barrier((blocks[6], blocks[7], main_block))
        main_moved = lax.all_to_all(main_moved, 'dap', 0, 0, tiled=True).reshape(size, -1, rows, main_block.shape[2])
        b_x, b_y = swap(b_to_x, XBIT, size), swap(b_to_y, YBIT, size)
        b_dx, b_dy = swap(b_y[hid // 2:2 * hid], XBIT, size), swap(b_x[hid:2 * hid + hid // 2], YBIT, size)
        b_parts = [b_to_x, b_to_y, b_x, b_y]
        b_parts = b_parts + [swap(part, CORE, size) for part in b_parts]
        b_parts = b_parts + [b_dx, b_dy, swap(b_dx, CORE, size), swap(b_dy, CORE, size)]
        near_tables, far_tables = (OWN_X, OWN_Y, FROM_X, FROM_Y), (FAR_X, FAR_Y)
        tables = tuple((bit, t) for ts in (near_tables, far_tables) for bit in (0, CORE) for t in ts)
        late = main_late(main_moved, mask_late, mg, mb, mwr, mbr)
        late_sib = swap(late, CORE, size)

        a_b, a_b_give, b_b = project(idx_b, [blocks[k] for k in SET_B], mask_seq, gamma, beta, w_both, bias, hid)
        a_b_sib, b_b_sib = swap(a_b_give, CORE, size), swap(b_b, CORE, size)
        fx, fy, nx, ny, kx, ky, own = extra_parts(me1, (a_a, a_a_sib, a_b, a_b_sib), (b_a, b_a_sib, b_b, b_b_sib), w_e, cols)
        fx, fy = swap(fx, XBIT, size), swap(fy, YBIT, size)
        nx, ny = swap(nx, XBIT, size), swap(ny, YBIT, size)
        kx = (kx.astype(F32) + fy.astype(F32)).astype(BF16)
        ky = (ky.astype(F32) + fx.astype(F32)).astype(BF16)
        kx, ky = swap(kx, XBIT, size), swap(ky, YBIT, size)

        base = main_rows(me1, a_m, b_parts, tables, (late, late_sib), w_m, bias_m, inv_m, pair_rows)
        main_out = assemble(main_moved)
        extra_out = turn_out(me1, blocks, (0, 1, 2, 3), size)
        extra_out = turn_out(me1, blocks, (4, 5, 6, 7), size, extra_out).transpose(0, 2, 1)
        base = combine(base, inv_e, nx, ny, own, bias_e)
        pair_out = combine(base, inv_e, ky, kx)
        return pair_out, extra_out, main_out

    in_specs = (value_spec, mask_spec, value_spec, mask_spec, row_spec) + (P(),) * 16
    return jax.shard_map(local_program, mesh=mesh, in_specs=in_specs, out_specs=(row_spec, row_spec, row_spec), check_vma=False)
```

```python
import functools

import jax
import jax.numpy as jnp
from jax import lax
from jax.experimental import pallas as pl
from jax.experimental.pallas import tpu as pltpu
from jax.sharding import PartitionSpec as P


LN_EPS = 1e-5
NORM_EPS = 1e-3
NT = (((1,), (1,)), ((), ()))
F32 = jnp.float32
BF16 = jnp.bfloat16
ANY = pl.BlockSpec(memory_space=pl.ANY)
CORE, XBIT, YBIT = 1, 2, 4
LANES = 128
NEAR, REST = (2, 4, 3, 5), (6, 7, 1, 0)


def swap(value, bit, size):
    return lax.ppermute(value, 'dap', [(d, d ^ bit) for d in range(size)])


def turn_kernel(ks, me_ref, x_ref, *refs):
    outs, (v, s_in, s_out) = refs[:len(ks)], refs[len(ks):]
    seqs = v.shape[3]
    loads = [
        pltpu.make_async_copy(x_ref.at[:, :, pl.ds(pl.multiple_of((me_ref[0] ^ k) * seqs, LANES), seqs)], v.at[t], s_in.at[t])
        for t, k in enumerate(ks)
    ]
    stores = [pltpu.make_async_copy(v.at[t], out, s_out.at[t]) for t, out in enumerate(outs)]
    for c in loads:
        c.start()
    for load, save in zip(loads, stores):
        load.wait()
        save.start()
    for c in stores:
        c.wait()


def turn(me, x, ks, size):
    rows, chans, total = x.shape
    seqs = total // size
    return pl.pallas_call(
        functools.partial(turn_kernel, ks),
        grid_spec=pltpu.PrefetchScalarGridSpec(
            num_scalar_prefetch=1,
            grid=(1,),
            in_specs=[ANY],
            out_specs=[ANY] * len(ks),
            scratch_shapes=[
                pltpu.VMEM((len(ks), rows, chans, seqs), x.dtype),
                pltpu.SemaphoreType.DMA((len(ks),)),
                pltpu.SemaphoreType.DMA((len(ks),)),
            ],
        ),
        out_shape=[jax.ShapeDtypeStruct((rows, chans, seqs), x.dtype) for _ in ks],
        cost_estimate=pl.CostEstimate(flops=1 << 24, bytes_accessed=4 << 20, transcendentals=0),
        name='turn',
    )(me, x)


def turn_out_kernel(ks, me_ref, *refs):
    x_refs, (out_ref, in_v, out_v) = refs[:len(ks)], refs[-3:]
    rows, lead = x_refs[0].shape[:2]
    for k, ref in zip(ks, x_refs):
        at = lax.rem(me_ref[0] ^ k, len(ks)) * rows
        in_v[pl.ds(pl.multiple_of(at, rows), rows)] = ref[...].astype(F32)
    for c in range(lead):
        out_v[:, c, :] = in_v[:, c, :].T
    out_ref[...] = out_v[...].astype(BF16)


def turn_out(me, blocks, ks, size, into=None, lead=16):
    rows, chans, seqs = blocks[ks[0]].shape
    res = rows * len(ks)
    halves = size // len(ks)
    carried = [] if into is None else [into]
    return pl.pallas_call(
        functools.partial(turn_out_kernel, ks),
        grid_spec=pltpu.PrefetchScalarGridSpec(
            num_scalar_prefetch=1,
            grid=(seqs // LANES, chans // lead),
            in_specs=[pl.BlockSpec((rows, lead, LANES), lambda k, c, i: (0, c, k)) for _ in ks] + [ANY] * len(carried),
            out_specs=pl.BlockSpec((LANES, lead, res), lambda k, c, i: (k, c, (i[0] ^ ks[0]) // len(ks))),
            scratch_shapes=[pltpu.VMEM((res, lead, LANES), F32), pltpu.VMEM((LANES, lead, res), F32)],
        ),
        out_shape=jax.ShapeDtypeStruct((seqs, chans, halves * res), BF16),
        input_output_aliases={len(ks) + 1: 0} if carried else {},
        cost_estimate=pl.CostEstimate(flops=1 << 24, bytes_accessed=13 << 20, transcendentals=0),
        name='turn_out',
    )(me, *[blocks[k] for k in ks], *carried)


def project_kernel(group, idx_ref, *refs):
    count = len(refs) - 12
    x_refs = refs[:count]
    mask_ref, gamma_ref, beta_ref, w_ref, bias_ref, own_ref, sib_ref, b_ref, x_v, a_v, s_in, s_out = refs[count:]
    rows, chans, seqs = x_v.shape[1:]
    hid = b_ref.shape[1]
    half = group * hid
    block = pl.program_id(0)
    slot = lax.rem(block, 2)
    loads = [pltpu.make_async_copy(ref, x_v.at[t], s_in.at[t]) for t, ref in enumerate(x_refs)]
    targets = [own_ref.at[t] for t in range(count // 2)] + [sib_ref.at[t] for t in range(count // 2)]
    saves = [pltpu.make_async_copy(a_v.at[t % 2], target, s_out.at[t % 2]) for t, target in enumerate(targets)]

    @pl.when(block == 0)
    def _():
        for c in loads:
            c.start()

    for t in range(count):
        @pl.when(block == t)
        def _(t=t):
            loads[t].wait()
            if t >= 2:
                saves[t - 2].wait()

    def body(step, carry):
        pieces = []
        for part in range(2):
            first = pl.multiple_of(step * 2 * group + part * group, group)
            x = x_v[block, pl.ds(first, group)].astype(F32)
            centered = x - jnp.mean(x, axis=1, keepdims=True)
            var = jnp.mean(centered * centered, axis=1, keepdims=True)
            y = centered * lax.rsqrt(var + LN_EPS) * gamma_ref[...][None] + beta_ref[...][None]
            y = y.astype(BF16).reshape(group * chans, seqs)
            z = jnp.dot(w_ref[...], y, preferred_element_type=F32) + bias_ref[...]
            mask = mask_ref[pl.ds(first, group), :]
            left = z[:half].reshape(group, hid, seqs) * mask[:, None, :]
            a_v[slot, pl.ds(pl.multiple_of(first * hid, half), half), :] = left.astype(BF16).reshape(half, seqs)
            pieces.append(z[half:].reshape(hid, group, seqs) * mask[None])
        both = jnp.concatenate(pieces, axis=1).astype(BF16)
        b_ref[0, :, pl.ds(pl.multiple_of(step * 2 * group, 2 * group), 2 * group), :] = both
        return carry

    lax.fori_loop(0, rows // (2 * group), body, 0)
    for t in range(count):
        @pl.when(block == t)
        def _(t=t):
            saves[t].start()
            if t == count - 1:
                for c in saves[t - 1:]:
                    c.wait()


def project_weights(w_left, b_left, w_right, b_right, seqs, group=8):
    chans, hid = w_left.shape
    eye = jnp.eye(group, dtype=BF16)
    w_a = jnp.einsum('gh,mp->gphm', eye, w_left).reshape(group * hid, group * chans)
    w_b = jnp.einsum('gh,mq->qghm', eye, w_right).reshape(group * hid, group * chans)
    w_both = jnp.concatenate([w_a, w_b], axis=0)
    bias = jnp.concatenate([jnp.tile(b_left, group), jnp.repeat(b_right, group)]).astype(F32)
    return w_both, jnp.broadcast_to(bias[:, None], (2 * group * hid, seqs))


def project(idx, blocks, mask_t, gamma, beta, w_both, bias, hid, group=8):
    count = len(blocks)
    rows, chans, seqs = blocks[0].shape
    whole = lambda v: pl.BlockSpec(v.shape, lambda s, i: (0,) * v.ndim)
    return pl.pallas_call(
        functools.partial(project_kernel, group),
        grid_spec=pltpu.PrefetchScalarGridSpec(
            num_scalar_prefetch=1,
            grid=(count,),
            in_specs=[ANY] * count + [
                pl.BlockSpec((rows, seqs), lambda s, i: (i[s], 0)),
                whole(gamma), whole(beta), whole(w_both), whole(bias),
            ],
            out_specs=[ANY, ANY, pl.BlockSpec((1, hid, rows, seqs), lambda s, i: (s, 0, 0, 0))],
            scratch_shapes=[
                pltpu.VMEM((count, rows, chans, seqs), BF16),
                pltpu.VMEM((2, rows * hid, seqs), BF16),
                pltpu.SemaphoreType.DMA((count,)),
                pltpu.SemaphoreType.DMA((2,)),
            ],
        ),
        out_shape=[
            jax.ShapeDtypeStruct((count // 2, rows * hid, seqs), BF16),
            jax.ShapeDtypeStruct((count // 2, rows * hid, seqs), BF16),
            jax.ShapeDtypeStruct((count, hid, rows, seqs), BF16),
        ],
        compiler_params=pltpu.CompilerParams(vmem_limit_bytes=48 << 20),
        cost_estimate=pl.CostEstimate(flops=6 << 30, bytes_accessed=13 << 20, transcendentals=0),
        name='project',
    )(idx, *blocks, mask_t, gamma, beta, w_both, bias)


def outer_rows(a, b_v, o_v, qu, ready=None, more=None):
    rows, hid, _, cols = o_v.shape

    def q_body(g, carry):
        if ready is not None:
            ready(g)
        for u in range(qu):
            q = g * qu + u
            o = lax.dot_general(a[...], b_v[q], NT, preferred_element_type=F32)
            if more is not None:
                o = o + jnp.dot(more[0][...], more[1][q], preferred_element_type=F32)
            o_v[:, q] = o.astype(BF16).reshape(rows, hid, cols)
        return carry

    lax.fori_loop(0, hid // qu, q_body, 0)


def weigh_rows(w_ref, o_v, iu, store):
    rows, hid, _, cols = o_v.shape

    def i_body(g, carry):
        for u in range(iu):
            i = g * iu + u
            store(i, jnp.dot(w_ref[...], o_v[i].reshape(hid * hid, cols), preferred_element_type=F32))
        return carry

    lax.fori_loop(0, rows // iu, i_body, 0)


SET_A, SET_B = (0, 2, 4, 1, 3, 5), (6, 7)


def extra_kernel(qu, iu, me_ref, *refs):
    (a_a, a_a_sib, a_b, a_b_sib), b_refs = refs[:4], refs[4:8]
    w_ref, fx, fy, nx, ny, kx, ky, own, a_v, b_v, o_v, r_v, sa, sb, so = refs[8:]
    step = pl.program_id(0)
    slot = lax.rem(step, 2)
    half = kx.shape[0]
    lo, hi = pl.ds(0, half), pl.ds(half, half)
    depth = a_a.shape[2]
    width = b_refs[0].shape[2]

    def a_copies(t):
        pair, at = (((a_b, a_b_sib), 0), ((a_a, a_a_sib), 1), ((a_a, a_a_sib), 2), ((a_a, a_a_sib), 0))[t]
        return [
            pltpu.make_async_copy(ref.at[at], a_v.at[t % 2, :, pl.ds(n * depth, depth)], sa.at[t % 2, n])
            for n, ref in enumerate(pair)
        ]

    def b_copies(g):
        out = []
        qs = pl.ds(g * qu, qu)
        pieces = [(n, ref, t, k) for n, (ref, ks) in enumerate(zip(b_refs, (SET_A, SET_A, SET_B, SET_B))) for t, k in enumerate(ks)]
        for m, (n, ref, t, k) in enumerate(pieces):
            k = k ^ CORE if n % 2 else k
            js = pl.ds(pl.multiple_of((me_ref[0] ^ k) * width, width), width)
            out.append(pltpu.make_async_copy(ref.at[t, qs], b_v.at[qs, js, pl.ds(n % 2 * depth, depth)], sb.at[g, m]))
        return out

    def out_copies(t):
        lower, upper = ((fx, fy), (nx, kx), (ky, ny), (own.at[lo], own.at[hi]))[t]
        sl = t % 2
        return [
            pltpu.make_async_copy(r_v.at[sl, lo], lower, so.at[sl, 0]),
            pltpu.make_async_copy(r_v.at[sl, hi], upper, so.at[sl, 1]),
        ]

    @pl.when(step == 0)
    def _():
        for c in a_copies(0):
            c.start()
        for g in range(b_v.shape[0] // qu):
            for c in b_copies(g):
                c.start()

    for t in range(4):
        @pl.when(step == t)
        def _(t=t):
            for c in a_copies(t):
                c.wait()
            if t < 3:
                for c in a_copies(t + 1):
                    c.start()

    def ready(g):
        @pl.when(step == 0)
        def _():
            for c in b_copies(g):
                c.wait()

    outer_rows(a_v.at[slot], b_v, o_v, qu, ready)
    for t in range(2, 4):
        @pl.when(step == t)
        def _(t=t):
            for c in out_copies(t - 2):
                c.wait()

    def store(i, r):
        r_v[slot, i] = r.astype(BF16)

    weigh_rows(w_ref, o_v, iu, store)
    for t in range(4):
        @pl.when(step == t)
        def _(t=t):
            for c in out_copies(t):
                c.start()
            if t == 3:
                for c in out_copies(2) + out_copies(3):
                    c.wait()


def turn_weights(w_out, hid):
    return w_out.reshape(hid, hid, -1).transpose(2, 1, 0).reshape(-1, hid * hid)


def extra_parts(me, a_parts, b_parts, w_t, cols, qu=8, iu=8):
    hid, depth = b_parts[0].shape[1], 2 * b_parts[0].shape[3]
    rows = a_parts[0].shape[1] // hid
    chans = w_t.shape[0]
    half = rows // 2
    part = lambda *lead: jax.ShapeDtypeStruct(lead + (chans, cols), BF16)
    return pl.pallas_call(
        functools.partial(extra_kernel, qu, iu),
        grid_spec=pltpu.PrefetchScalarGridSpec(
            num_scalar_prefetch=1,
            grid=(4,),
            in_specs=[ANY] * 8 + [pl.BlockSpec(w_t.shape, lambda s, i: (0, 0))],
            out_specs=[ANY] * 7,
            scratch_shapes=[
                pltpu.VMEM((2, rows * hid, depth), BF16),
                pltpu.VMEM((hid, cols, depth), BF16),
                pltpu.VMEM((rows, hid, hid, cols), BF16),
                pltpu.VMEM((2, rows, chans, cols), BF16),
                pltpu.SemaphoreType.DMA((2, 2)),
                pltpu.SemaphoreType.DMA((hid // qu, 16)),
                pltpu.SemaphoreType.DMA((2, 2)),
            ],
        ),
        out_shape=[part(half)] * 6 + [part(rows)],
        compiler_params=pltpu.CompilerParams(vmem_limit_bytes=60 << 20),
        cost_estimate=pl.CostEstimate(flops=60 << 30, bytes_accessed=32 << 20, transcendentals=0),
        name='extra_outer',
    )(me, *a_parts, *b_parts, w_t)


def main_late_kernel(x_ref, mask_ref, gamma_ref, beta_ref, w_ref, bias_ref, out_ref, z_v):
    srcs, seqs, rows, chans = x_ref.shape
    hid = w_ref.shape[0]

    def body(g, carry):
        for u in range(4):
            n = g * 4 + u
            x = x_ref[:, n].reshape(srcs * rows, chans).astype(F32)
            centered = x - jnp.mean(x, axis=1, keepdims=True)
            var = jnp.mean(centered * centered, axis=1, keepdims=True)
            y = (centered * lax.rsqrt(var + LN_EPS) * gamma_ref[...] + beta_ref[...]).astype(BF16)
            z = lax.dot_general(w_ref[...], y, NT, preferred_element_type=F32) + bias_ref[...]
            z_v[n] = z * mask_ref[pl.ds(n, 1), :]
        return carry

    lax.fori_loop(0, seqs // 4, body, 0)
    for q in range(hid):
        out_ref[q] = z_v[:, q, :].astype(BF16)


def main_late(moved, mask, gamma, beta, w_right, b_right, block=16):
    srcs, seqs, rows, chans = moved.shape
    hid = w_right.shape[1]
    res = srcs * rows
    whole = lambda v: pl.BlockSpec(v.shape, lambda s: (0,) * v.ndim)
    row = lambda v: v.astype(F32)[None]
    bias = jnp.broadcast_to(b_right.astype(F32)[:, None], (hid, res))
    args = (row(gamma), row(beta), w_right.T, bias)
    return pl.pallas_call(
        main_late_kernel,
        grid=(seqs // block,),
        in_specs=[
            pl.BlockSpec((srcs, block, rows, chans), lambda s: (0, s, 0, 0)),
            pl.BlockSpec((block, res), lambda s: (s, 0)),
        ] + [whole(v) for v in args],
        out_specs=pl.BlockSpec((hid, block, res), lambda s: (0, s, 0)),
        out_shape=jax.ShapeDtypeStruct((hid, seqs, res), BF16),
        scratch_shapes=[pltpu.VMEM((block, hid, res), F32)],
        compiler_params=pltpu.CompilerParams(vmem_limit_bytes=32 << 20),
        cost_estimate=pl.CostEstimate(flops=4 << 30, bytes_accessed=10 << 20, transcendentals=0),
        name='main_late',
    )(moved, mask, *args)


HID = 32
OWN_X = ((0, HID, 0, 0, 3), (HID, HID, 0, 0, 2))
OWN_Y = ((HID, HID, 0, 0, 1),)
FROM_X = ((0, HID, XBIT, 0, 2), (HID, HID, XBIT, 0, 3), (2 * HID, HID, XBIT, 0, 1))
FROM_Y = ((0, HID, YBIT, 0, 2), (HID, HID, YBIT, 0, 3), (2 * HID, HID, YBIT, 0, 1))
FAR_Y = ((0, HID, XBIT | YBIT, 0, 1), (HID, HID // 2, XBIT | YBIT, 0, 3))
FAR_X = ((0, HID // 2, XBIT | YBIT, HID // 2, 3), (HID // 2, HID, XBIT | YBIT, 0, 2))


def main_kernel(tables, qu, iu, idx_ref, a_ref, *refs):
    b_refs, late_refs = refs[:len(tables)], refs[len(tables):len(tables) + 2]
    w_ref, bias_ref, inv_ref, z_ref, out_ref, a_v, c_v, b_v, l_v, o_v, sa, sb = refs[len(tables) + 2:]
    me = idx_ref[0]
    chip, core = me // 2, lax.rem(me, 2)
    lanes = lambda n: pl.ds(pl.multiple_of(n * LANES, LANES), LANES)
    first_copies = []
    for r in range(4):
        target = c_v if r == 0 else a_v.at[:, lanes(r - 1)]
        first_copies.append(pltpu.make_async_copy(a_ref.at[:, lanes(chip ^ r)], target, sa.at[r]))
    for n, ref in enumerate(late_refs):
        seqs = ref.shape[1]
        at = pl.ds(pl.multiple_of((core ^ n) * seqs, seqs), seqs)
        first_copies.append(pltpu.make_async_copy(ref, l_v.at[:, at, :], sa.at[4 + n]))
    width = b_refs[0].shape[1]
    groups = b_v.shape[0] // qu
    b_copies = [[] for _ in range(groups)]
    for ref, (core_bit, table) in zip(b_refs, tables):
        for first, rows, k, q, r in table:
            js = pl.ds(pl.multiple_of((me ^ k ^ core_bit) * width, width), width)
            for part in range(rows // qu):
                src = ref.at[pl.ds(first + part * qu, qu)]
                g = q // qu + part
                b_copies[g].append(pltpu.make_async_copy(src, b_v.at[pl.ds(g * qu, qu), js, lanes(r - 1)], sb.at[g, len(b_copies[g])]))
    for c in first_copies + [c for group in b_copies for c in group]:
        c.start()
    for c in first_copies:
        c.wait()

    def ready(g):
        for n in range(groups):
            @pl.when(g == n)
            def _(n=n):
                for c in b_copies[n]:
                    c.wait()

    outer_rows(a_v, b_v, o_v, qu, ready=ready, more=(c_v, l_v))

    def store(i, r):
        out_ref[i] = z_ref[i] + ((r + bias_ref[...]) * inv_ref[pl.ds(i, 1), :]).T

    weigh_rows(w_ref, o_v, iu, store)


def main_rows(me, a, b_parts, tables, late, w_t, bias, inv, z, qu=8, iu=8):
    rows, cols, _ = z.shape
    hid = a.shape[0] // rows
    pieces = sum(piece[1] for _, table in tables for piece in table) // hid
    whole = lambda v: pl.BlockSpec(v.shape, lambda s, i: (0,) * v.ndim)
    return pl.pallas_call(
        functools.partial(main_kernel, tables, qu, iu),
        grid_spec=pltpu.PrefetchScalarGridSpec(
            num_scalar_prefetch=1,
            grid=(1,),
            in_specs=[ANY] * (len(b_parts) + 3) + [whole(w_t), whole(bias), whole(inv), whole(z)],
            out_specs=whole(z),
            scratch_shapes=[
                pltpu.VMEM((rows * hid, 3 * LANES), BF16),
                pltpu.VMEM((rows * hid, LANES), BF16),
                pltpu.VMEM((hid, cols, 3 * LANES), BF16),
                pltpu.VMEM((hid, LANES, cols), BF16),
                pltpu.VMEM((rows, hid, hid, cols), BF16),
                pltpu.SemaphoreType.DMA((6,)),
                pltpu.SemaphoreType.DMA((hid // qu, pieces)),
            ],
        ),
        out_shape=jax.ShapeDtypeStruct(z.shape, F32),
        compiler_params=pltpu.CompilerParams(vmem_limit_bytes=48 << 20),
        cost_estimate=pl.CostEstimate(flops=12 << 30, bytes_accessed=20 << 20, transcendentals=0),
        name='main_outer',
    )(me, a, *b_parts, *late, w_t, bias, inv, z)


def combine_kernel(base_ref, inv_ref, lower_ref, upper_ref, *refs):
    step = pl.program_id(0)
    out_ref = refs[-1]

    def add(ref):
        for i in range(out_ref.shape[0]):
            total = ref[i].astype(F32)
            if len(refs) > 1:
                total = total + refs[0][i].astype(F32) + refs[1][...]
            row = step * out_ref.shape[0] + i
            out_ref[i] = base_ref[i] + (total * inv_ref[pl.ds(row, 1), :]).T

    @pl.when(step < pl.num_programs(0) // 2)
    def _():
        add(lower_ref)

    @pl.when(step >= pl.num_programs(0) // 2)
    def _():
        add(upper_ref)


def combine(base, inv, lower, upper, own=None, bias=None, block=16):
    rows, cols, chans = base.shape
    mid = rows // block // 2
    flat = lambda: pl.BlockSpec((block, cols, chans), lambda s: (s, 0, 0))
    extra, extra_specs = (), []
    if own is not None:
        extra = (own, bias)
        extra_specs = [pl.BlockSpec((block, chans, cols), lambda s: (s, 0, 0)), pl.BlockSpec((chans, cols), lambda s: (0, 0))]
    return pl.pallas_call(
        combine_kernel,
        grid=(2 * mid,),
        in_specs=[
            flat(),
            pl.BlockSpec((rows, cols), lambda s: (0, 0)),
            pl.BlockSpec((block, chans, cols), lambda s: (jnp.minimum(s, mid - 1), 0, 0)),
            pl.BlockSpec((block, chans, cols), lambda s: (jnp.maximum(s - mid, 0), 0, 0)),
        ] + extra_specs,
        out_specs=flat(),
        out_shape=jax.ShapeDtypeStruct(base.shape, F32),
        compiler_params=pltpu.CompilerParams(vmem_limit_bytes=24 << 20),
        cost_estimate=pl.CostEstimate(flops=1 << 24, bytes_accessed=15 << 20, transcendentals=0),
        name='combine',
    )(base, inv, lower, upper, *extra)


def assemble_kernel(ref, out_ref):
    width = ref.shape[2]
    for d in range(ref.shape[0]):
        out_ref[:, d * width:(d + 1) * width, :] = ref[d]


def assemble(value, block=8):
    srcs, seqs, width, chans = value.shape
    return pl.pallas_call(
        assemble_kernel,
        grid=(seqs // block,),
        in_specs=[pl.BlockSpec((srcs, block, width, chans), lambda s: (0, s, 0, 0))],
        out_specs=pl.BlockSpec((block, srcs * width, chans), lambda s: (s, 0, 0)),
        out_shape=jax.ShapeDtypeStruct((seqs, srcs * width, chans), value.dtype),
        cost_estimate=pl.CostEstimate(flops=1 << 24, bytes_accessed=16 << 20, transcendentals=0),
        name='assemble',
    )(value)


def layer_norm(value, gamma, beta):
    as_float = value.astype(F32)
    mean = jnp.mean(as_float, axis=-1, keepdims=True)
    centered = as_float - mean
    var = jnp.mean(centered * centered, axis=-1, keepdims=True)
    return (centered * lax.rsqrt(var + LN_EPS) * gamma.astype(F32) + beta.astype(F32)).astype(BF16)


def inverse_norms(mask, mask_rows):
    counts = jnp.einsum('si,sj->ij', mask_rows.astype(BF16), mask.astype(BF16), preferred_element_type=F32)
    return 1.0 / (NORM_EPS + counts)


def solution(mesh):
    size = mesh.shape['dap']
    value_spec = P('data', 'dap', None)
    mask_spec = P('data', None)
    row_spec = P(('data', 'dap'), None, None)

    def local_program(extra_block, extra_mask, main_block, main_mask, pair_rows, eg, eb, ewl, ebl, ewr, ebr, ewo, ebo, mg, mb, mwl, mbl, mwr, mbr, mwo, mbo):
        me = lax.axis_index('dap')
        chip = me // 2
        rows = extra_block.shape[1]
        hid = ewl.shape[1]

        seqs = extra_block.shape[0] // size
        cols = size * rows
        minor = extra_block.transpose(1, 2, 0)
        me1 = me.astype(jnp.int32)[None]
        turned = dict(zip(NEAR[:2], turn(me1, minor, NEAR[:2], size)))
        turned.update(zip(NEAR[2:], turn(me1, minor, NEAR[2:], size)))
        turned.update(zip(REST, turn(me1, minor, REST, size)))
        blocks = {0: turned[0]}
        for k in NEAR[:2]:
            blocks[k] = swap(turned[k], k, size)
        for k in NEAR[2:]:
            blocks[k] = swap(turned[k], k, size)
        blocks[1] = swap(turned[1], CORE, size)
        near, far = lax.optimization_barrier(([blocks[k] for k in NEAR], [turned[6], turned[7]]))
        blocks.update(zip(NEAR, near))
        for k, value in zip((6, 7), far):
            blocks[k] = swap(value, k, size)

        mask_rows_m = lax.dynamic_slice_in_dim(main_mask, me * rows, rows, axis=1)
        normed = layer_norm(main_block, mg, mb)
        mask_m = mask_rows_m.astype(F32).T

        wide = lambda v, n: jnp.broadcast_to(v.astype(F32)[:, None], (v.shape[0], n))
        mask_seq = lax.dynamic_slice_in_dim(extra_mask, me * seqs, seqs, axis=0).astype(F32).T
        w_both, bias = project_weights(ewl, ebl, ewr, ebr, seqs)
        gamma, beta = wide(eg, seqs), wide(eb, seqs)
        idx_a, idx_b = [(me ^ jnp.array(ks, jnp.int32)).astype(jnp.int32) for ks in (SET_A, SET_B)]
        a_m = jnp.einsum('sim,mp->ips', normed, mwl, preferred_element_type=F32) + mbl.astype(F32)[None, :, None]
        a_m = (a_m * mask_m[:, None, :]).astype(BF16).reshape(rows * hid, -1)
        b_m = jnp.einsum('sim,mq->qis', normed, mwr, preferred_element_type=F32) + mbr.astype(F32)[:, None, None]
        b_m = (b_m * mask_m[None]).astype(BF16)
        pick = lambda r: lax.dynamic_slice_in_dim(b_m, (chip ^ r) * LANES, LANES, axis=2)
        b_0, b_1, b_2, b_3 = [pick(r) for r in range(4)]
        b_to_x, b_to_y = jnp.concatenate([b_3, b_2, b_0]), jnp.concatenate([b_0, b_1, b_3])
        mask_rows_e = lax.dynamic_slice_in_dim(extra_mask, me * rows, rows, axis=1)
        inv_m = inverse_norms(main_mask, mask_rows_m)
        inv_e = inverse_norms(extra_mask, mask_rows_e)
        w_e, w_m = turn_weights(ewo, hid), turn_weights(mwo, hid)
        bias_e, bias_m = wide(ebo, cols), wide(mbo, cols)
        count = main_mask.shape[0] // size
        mask_late = lax.dynamic_slice_in_dim(main_mask, me * count, count, axis=0).astype(F32)

        a_a, a_a_give, b_a = project(idx_a, [blocks[k] for k in SET_A], mask_seq, gamma, beta, w_both, bias, hid)
        a_a_sib, b_a_sib = swap(a_a_give, CORE, size), swap(b_a, CORE, size)

        blocks[6], blocks[7], main_moved = lax.optimization_barrier((blocks[6], blocks[7], main_block))
        main_moved = lax.all_to_all(main_moved, 'dap', 0, 0, tiled=True).reshape(size, -1, rows, main_block.shape[2])
        b_x, b_y = swap(b_to_x, XBIT, size), swap(b_to_y, YBIT, size)
        b_dx, b_dy = swap(b_y[hid // 2:2 * hid], XBIT, size), swap(b_x[hid:2 * hid + hid // 2], YBIT, size)
        b_parts = [b_to_x, b_to_y, b_x, b_y]
        b_parts = b_parts + [swap(part, CORE, size) for part in b_parts]
        b_parts = b_parts + [b_dx, b_dy, swap(b_dx, CORE, size), swap(b_dy, CORE, size)]
        near_tables, far_tables = (OWN_X, OWN_Y, FROM_X, FROM_Y), (FAR_X, FAR_Y)
        tables = tuple((bit, t) for ts in (near_tables, far_tables) for bit in (0, CORE) for t in ts)
        late = main_late(main_moved, mask_late, mg, mb, mwr, mbr)
        late_sib = swap(late, CORE, size)

        a_b, a_b_give, b_b = project(idx_b, [blocks[k] for k in SET_B], mask_seq, gamma, beta, w_both, bias, hid)
        a_b_sib, b_b_sib = swap(a_b_give, CORE, size), swap(b_b, CORE, size)
        fx, fy, nx, ny, kx, ky, own = extra_parts(me1, (a_a, a_a_sib, a_b, a_b_sib), (b_a, b_a_sib, b_b, b_b_sib), w_e, cols)
        fx, fy = swap(fx, XBIT, size), swap(fy, YBIT, size)
        nx, ny = swap(nx, XBIT, size), swap(ny, YBIT, size)
        kx = (kx.astype(F32) + fy.astype(F32)).astype(BF16)
        ky = (ky.astype(F32) + fx.astype(F32)).astype(BF16)
        kx, ky = swap(kx, XBIT, size), swap(ky, YBIT, size)

        base = main_rows(me1, a_m, b_parts, tables, (late, late_sib), w_m, bias_m, inv_m, pair_rows)
        main_out = assemble(main_moved)
        extra_out = turn_out(me1, blocks, (0, 1, 2, 3), size)
        extra_out = turn_out(me1, blocks, (4, 5, 6, 7), size, extra_out).transpose(0, 2, 1)
        base = combine(base, inv_e, nx, ny, own, bias_e)
        pair_out = combine(base, inv_e, ky, kx)
        return pair_out, extra_out, main_out

    in_specs = (value_spec, mask_spec, value_spec, mask_spec, row_spec) + (P(),) * 16
    return jax.shard_map(local_program, mesh=mesh, in_specs=in_specs, out_specs=(row_spec, row_spec, row_spec), check_vma=False)
```

```python
import functools

import jax
import jax.numpy as jnp
from jax import lax
from jax.experimental import pallas as pl
from jax.experimental.pallas import tpu as pltpu
from jax.sharding import PartitionSpec as P


LN_EPS = 1e-5
NORM_EPS = 1e-3
NT = (((1,), (1,)), ((), ()))
F32 = jnp.float32
BF16 = jnp.bfloat16
ANY = pl.BlockSpec(memory_space=pl.ANY)
CORE, XBIT, YBIT = 1, 2, 4
LANES = 128
PIECES = 4
NEAR, REST = (2, 4, 3, 5), (6, 7, 1, 0)


def swap(value, bit, size):
    return lax.ppermute(value, 'dap', [(d, d ^ bit) for d in range(size)])


def turn_kernel(ks, me_ref, x_ref, *refs):
    outs, (v, s_in, s_out) = refs[:len(ks)], refs[len(ks):]
    seqs = v.shape[3]
    rows = v.shape[1] // PIECES
    loads, stores = [], []
    for n in range(len(ks) * PIECES):
        t, piece = divmod(n, PIECES)
        at = pl.ds(piece * rows, rows)
        lanes = pl.ds(pl.multiple_of((me_ref[0] ^ ks[t]) * seqs, LANES), seqs)
        loads.append(pltpu.make_async_copy(x_ref.at[at, :, lanes], v.at[t, at], s_in.at[n]))
        stores.append(pltpu.make_async_copy(v.at[t, at], outs[t].at[at], s_out.at[n]))
    for c in loads:
        c.start()
    for load, save in zip(loads, stores):
        load.wait()
        save.start()
    for c in stores:
        c.wait()


def turn(me, x, ks, size):
    rows, chans, total = x.shape
    seqs = total // size
    return pl.pallas_call(
        functools.partial(turn_kernel, ks),
        grid_spec=pltpu.PrefetchScalarGridSpec(
            num_scalar_prefetch=1,
            grid=(1,),
            in_specs=[ANY],
            out_specs=[ANY] * len(ks),
            scratch_shapes=[
                pltpu.VMEM((len(ks), rows, chans, seqs), x.dtype),
                pltpu.SemaphoreType.DMA((len(ks) * PIECES,)),
                pltpu.SemaphoreType.DMA((len(ks) * PIECES,)),
            ],
        ),
        out_shape=[jax.ShapeDtypeStruct((rows, chans, seqs), x.dtype) for _ in ks],
        cost_estimate=pl.CostEstimate(flops=1 << 24, bytes_accessed=4 << 20, transcendentals=0),
        name='turn',
    )(me, x)


def turn_out_kernel(ks, me_ref, *refs):
    x_refs, (out_ref, in_v, out_v) = refs[:len(ks)], refs[-3:]
    rows, lead = x_refs[0].shape[:2]
    for k, ref in zip(ks, x_refs):
        at = lax.rem(me_ref[0] ^ k, len(ks)) * rows
        in_v[pl.ds(pl.multiple_of(at, rows), rows)] = ref[...].astype(F32)
    for c in range(lead):
        out_v[:, c, :] = in_v[:, c, :].T
    out_ref[...] = out_v[...].astype(BF16)


def turn_out(me, blocks, ks, size, into=None, lead=16):
    rows, chans, seqs = blocks[ks[0]].shape
    res = rows * len(ks)
    halves = size // len(ks)
    carried = [] if into is None else [into]
    return pl.pallas_call(
        functools.partial(turn_out_kernel, ks),
        grid_spec=pltpu.PrefetchScalarGridSpec(
            num_scalar_prefetch=1,
            grid=(seqs // LANES, chans // lead),
            in_specs=[pl.BlockSpec((rows, lead, LANES), lambda k, c, i: (0, c, k)) for _ in ks] + [ANY] * len(carried),
            out_specs=pl.BlockSpec((LANES, lead, res), lambda k, c, i: (k, c, (i[0] ^ ks[0]) // len(ks))),
            scratch_shapes=[pltpu.VMEM((res, lead, LANES), F32), pltpu.VMEM((LANES, lead, res), F32)],
        ),
        out_shape=jax.ShapeDtypeStruct((seqs, chans, halves * res), BF16),
        input_output_aliases={len(ks) + 1: 0} if carried else {},
        cost_estimate=pl.CostEstimate(flops=1 << 24, bytes_accessed=13 << 20, transcendentals=0),
        name='turn_out',
    )(me, *[blocks[k] for k in ks], *carried)


def project_kernel(group, idx_ref, *refs):
    count = len(refs) - 12
    x_refs = refs[:count]
    mask_ref, gamma_ref, beta_ref, w_ref, bias_ref, own_ref, sib_ref, b_ref, x_v, a_v, s_in, s_out = refs[count:]
    rows, chans, seqs = x_v.shape[1:]
    hid = b_ref.shape[1]
    half = group * hid
    block = pl.program_id(0)
    slot = lax.rem(block, 2)
    loads = [pltpu.make_async_copy(ref, x_v.at[t], s_in.at[t]) for t, ref in enumerate(x_refs)]
    targets = [own_ref.at[t] for t in range(count // 2)] + [sib_ref.at[t] for t in range(count // 2)]
    saves = [pltpu.make_async_copy(a_v.at[t % 2], target, s_out.at[t % 2]) for t, target in enumerate(targets)]

    @pl.when(block == 0)
    def _():
        for c in loads:
            c.start()

    for t in range(count):
        @pl.when(block == t)
        def _(t=t):
            loads[t].wait()
            if t >= 2:
                saves[t - 2].wait()

    def body(step, carry):
        pieces = []
        for part in range(2):
            first = pl.multiple_of(step * 2 * group + part * group, group)
            x = x_v[block, pl.ds(first, group)].astype(F32)
            centered = x - jnp.mean(x, axis=1, keepdims=True)
            var = jnp.mean(centered * centered, axis=1, keepdims=True)
            y = centered * lax.rsqrt(var + LN_EPS) * gamma_ref[...][None] + beta_ref[...][None]
            y = y.astype(BF16).reshape(group * chans, seqs)
            z = jnp.dot(w_ref[...], y, preferred_element_type=F32) + bias_ref[...]
            mask = mask_ref[pl.ds(first, group), :]
            left = z[:half].reshape(group, hid, seqs) * mask[:, None, :]
            a_v[slot, pl.ds(pl.multiple_of(first * hid, half), half), :] = left.astype(BF16).reshape(half, seqs)
            pieces.append(z[half:].reshape(hid, group, seqs) * mask[None])
        both = jnp.concatenate(pieces, axis=1).astype(BF16)
        b_ref[0, :, pl.ds(pl.multiple_of(step * 2 * group, 2 * group), 2 * group), :] = both
        return carry

    lax.fori_loop(0, rows // (2 * group), body, 0)
    for t in range(count):
        @pl.when(block == t)
        def _(t=t):
            saves[t].start()
            if t == count - 1:
                for c in saves[t - 1:]:
                    c.wait()


def project_weights(w_left, b_left, w_right, b_right, seqs, group=8):
    chans, hid = w_left.shape
    eye = jnp.eye(group, dtype=BF16)
    w_a = jnp.einsum('gh,mp->gphm', eye, w_left).reshape(group * hid, group * chans)
    w_b = jnp.einsum('gh,mq->qghm', eye, w_right).reshape(group * hid, group * chans)
    w_both = jnp.concatenate([w_a, w_b], axis=0)
    bias = jnp.concatenate([jnp.tile(b_left, group), jnp.repeat(b_right, group)]).astype(F32)
    return w_both, jnp.broadcast_to(bias[:, None], (2 * group * hid, seqs))


def project(idx, blocks, mask_t, gamma, beta, w_both, bias, hid, group=8):
    count = len(blocks)
    rows, chans, seqs = blocks[0].shape
    whole = lambda v: pl.BlockSpec(v.shape, lambda s, i: (0,) * v.ndim)
    return pl.pallas_call(
        functools.partial(project_kernel, group),
        grid_spec=pltpu.PrefetchScalarGridSpec(
            num_scalar_prefetch=1,
            grid=(count,),
            in_specs=[ANY] * count + [
                pl.BlockSpec((rows, seqs), lambda s, i: (i[s], 0)),
                whole(gamma), whole(beta), whole(w_both), whole(bias),
            ],
            out_specs=[ANY, ANY, pl.BlockSpec((1, hid, rows, seqs), lambda s, i: (s, 0, 0, 0))],
            scratch_shapes=[
                pltpu.VMEM((count, rows, chans, seqs), BF16),
                pltpu.VMEM((2, rows * hid, seqs), BF16),
                pltpu.SemaphoreType.DMA((count,)),
                pltpu.SemaphoreType.DMA((2,)),
            ],
        ),
        out_shape=[
            jax.ShapeDtypeStruct((count // 2, rows * hid, seqs), BF16),
            jax.ShapeDtypeStruct((count // 2, rows * hid, seqs), BF16),
            jax.ShapeDtypeStruct((count, hid, rows, seqs), BF16),
        ],
        compiler_params=pltpu.CompilerParams(vmem_limit_bytes=48 << 20),
        cost_estimate=pl.CostEstimate(flops=6 << 30, bytes_accessed=13 << 20, transcendentals=0),
        name='project',
    )(idx, *blocks, mask_t, gamma, beta, w_both, bias)


def outer_rows(a, b_v, o_v, qu, ready=None, more=None):
    rows, hid, _, cols = o_v.shape

    def q_body(g, carry):
        if ready is not None:
            ready(g)
        for u in range(qu):
            q = g * qu + u
            o = lax.dot_general(a[...], b_v[q], NT, preferred_element_type=F32)
            if more is not None:
                o = o + jnp.dot(more[0][...], more[1][q], preferred_element_type=F32)
            o_v[:, q] = o.astype(BF16).reshape(rows, hid, cols)
        return carry

    lax.fori_loop(0, hid // qu, q_body, 0)


def weigh_rows(w_ref, o_v, iu, store):
    rows, hid, _, cols = o_v.shape

    def i_body(g, carry):
        for u in range(iu):
            i = g * iu + u
            store(i, jnp.dot(w_ref[...], o_v[i].reshape(hid * hid, cols), preferred_element_type=F32))
        return carry

    lax.fori_loop(0, rows // iu, i_body, 0)


SET_A, SET_B = (0, 2, 4, 1, 3, 5), (6, 7)


def extra_kernel(qu, iu, me_ref, *refs):
    (a_a, a_a_sib, a_b, a_b_sib), b_refs = refs[:4], refs[4:8]
    w_ref, fx, fy, nx, ny, kx, ky, own, a_v, b_v, o_v, r_v, sa, sb, so = refs[8:]
    step = pl.program_id(0)
    slot = lax.rem(step, 2)
    half = kx.shape[0]
    lo, hi = pl.ds(0, half), pl.ds(half, half)
    depth = a_a.shape[2]
    width = b_refs[0].shape[2]

    def a_copies(t):
        pair, at = (((a_b, a_b_sib), 0), ((a_a, a_a_sib), 1), ((a_a, a_a_sib), 2), ((a_a, a_a_sib), 0))[t]
        return [
            pltpu.make_async_copy(ref.at[at], a_v.at[t % 2, :, pl.ds(n * depth, depth)], sa.at[t % 2, n])
            for n, ref in enumerate(pair)
        ]

    def b_copies(g):
        out = []
        qs = pl.ds(g * qu, qu)
        pieces = [(n, ref, t, k) for n, (ref, ks) in enumerate(zip(b_refs, (SET_A, SET_A, SET_B, SET_B))) for t, k in enumerate(ks)]
        for m, (n, ref, t, k) in enumerate(pieces):
            k = k ^ CORE if n % 2 else k
            js = pl.ds(pl.multiple_of((me_ref[0] ^ k) * width, width), width)
            out.append(pltpu.make_async_copy(ref.at[t, qs], b_v.at[qs, js, pl.ds(n % 2 * depth, depth)], sb.at[g, m]))
        return out

    def out_copies(t):
        lower, upper = ((fx, fy), (nx, kx), (ky, ny), (own.at[lo], own.at[hi]))[t]
        sl = t % 2
        return [
            pltpu.make_async_copy(r_v.at[sl, lo], lower, so.at[sl, 0]),
            pltpu.make_async_copy(r_v.at[sl, hi], upper, so.at[sl, 1]),
        ]

    @pl.when(step == 0)
    def _():
        for c in a_copies(0):
            c.start()
        for g in range(b_v.shape[0] // qu):
            for c in b_copies(g):
                c.start()

    for t in range(4):
        @pl.when(step == t)
        def _(t=t):
            for c in a_copies(t):
                c.wait()
            if t < 3:
                for c in a_copies(t + 1):
                    c.start()

    def ready(g):
        @pl.when(step == 0)
        def _():
            for c in b_copies(g):
                c.wait()

    outer_rows(a_v.at[slot], b_v, o_v, qu, ready)
    for t in range(2, 4):
        @pl.when(step == t)
        def _(t=t):
            for c in out_copies(t - 2):
                c.wait()

    def store(i, r):
        r_v[slot, i] = r.astype(BF16)

    weigh_rows(w_ref, o_v, iu, store)
    for t in range(4):
        @pl.when(step == t)
        def _(t=t):
            for c in out_copies(t):
                c.start()
            if t == 3:
                for c in out_copies(2) + out_copies(3):
                    c.wait()


def turn_weights(w_out, hid):
    return w_out.reshape(hid, hid, -1).transpose(2, 1, 0).reshape(-1, hid * hid)


def extra_parts(me, a_parts, b_parts, w_t, cols, qu=8, iu=8):
    hid, depth = b_parts[0].shape[1], 2 * b_parts[0].shape[3]
    rows = a_parts[0].shape[1] // hid
    chans = w_t.shape[0]
    half = rows // 2
    part = lambda *lead: jax.ShapeDtypeStruct(lead + (chans, cols), BF16)
    return pl.pallas_call(
        functools.partial(extra_kernel, qu, iu),
        grid_spec=pltpu.PrefetchScalarGridSpec(
            num_scalar_prefetch=1,
            grid=(4,),
            in_specs=[ANY] * 8 + [pl.BlockSpec(w_t.shape, lambda s, i: (0, 0))],
            out_specs=[ANY] * 7,
            scratch_shapes=[
                pltpu.VMEM((2, rows * hid, depth), BF16),
                pltpu.VMEM((hid, cols, depth), BF16),
                pltpu.VMEM((rows, hid, hid, cols), BF16),
                pltpu.VMEM((2, rows, chans, cols), BF16),
                pltpu.SemaphoreType.DMA((2, 2)),
                pltpu.SemaphoreType.DMA((hid // qu, 16)),
                pltpu.SemaphoreType.DMA((2, 2)),
            ],
        ),
        out_shape=[part(half)] * 6 + [part(rows)],
        compiler_params=pltpu.CompilerParams(vmem_limit_bytes=60 << 20),
        cost_estimate=pl.CostEstimate(flops=60 << 30, bytes_accessed=32 << 20, transcendentals=0),
        name='extra_outer',
    )(me, *a_parts, *b_parts, w_t)


def main_late_kernel(x_ref, mask_ref, gamma_ref, beta_ref, w_ref, bias_ref, out_ref, z_v):
    srcs, seqs, rows, chans = x_ref.shape
    hid = w_ref.shape[0]

    def body(g, carry):
        for u in range(4):
            n = g * 4 + u
            x = x_ref[:, n].reshape(srcs * rows, chans).astype(F32)
            centered = x - jnp.mean(x, axis=1, keepdims=True)
            var = jnp.mean(centered * centered, axis=1, keepdims=True)
            y = (centered * lax.rsqrt(var + LN_EPS) * gamma_ref[...] + beta_ref[...]).astype(BF16)
            z = lax.dot_general(w_ref[...], y, NT, preferred_element_type=F32) + bias_ref[...]
            z_v[n] = z * mask_ref[pl.ds(n, 1), :]
        return carry

    lax.fori_loop(0, seqs // 4, body, 0)
    for q in range(hid):
        out_ref[q] = z_v[:, q, :].astype(BF16)


def main_late(moved, mask, gamma, beta, w_right, b_right, block=16):
    srcs, seqs, rows, chans = moved.shape
    hid = w_right.shape[1]
    res = srcs * rows
    whole = lambda v: pl.BlockSpec(v.shape, lambda s: (0,) * v.ndim)
    row = lambda v: v.astype(F32)[None]
    bias = jnp.broadcast_to(b_right.astype(F32)[:, None], (hid, res))
    args = (row(gamma), row(beta), w_right.T, bias)
    return pl.pallas_call(
        main_late_kernel,
        grid=(seqs // block,),
        in_specs=[
            pl.BlockSpec((srcs, block, rows, chans), lambda s: (0, s, 0, 0)),
            pl.BlockSpec((block, res), lambda s: (s, 0)),
        ] + [whole(v) for v in args],
        out_specs=pl.BlockSpec((hid, block, res), lambda s: (0, s, 0)),
        out_shape=jax.ShapeDtypeStruct((hid, seqs, res), BF16),
        scratch_shapes=[pltpu.VMEM((block, hid, res), F32)],
        compiler_params=pltpu.CompilerParams(vmem_limit_bytes=32 << 20),
        cost_estimate=pl.CostEstimate(flops=4 << 30, bytes_accessed=10 << 20, transcendentals=0),
        name='main_late',
    )(moved, mask, *args)


HID = 32
OWN_X = ((0, HID, 0, 0, 3), (HID, HID, 0, 0, 2))
OWN_Y = ((HID, HID, 0, 0, 1),)
FROM_X = ((0, HID, XBIT, 0, 2), (HID, HID, XBIT, 0, 3), (2 * HID, HID, XBIT, 0, 1))
FROM_Y = ((0, HID, YBIT, 0, 2), (HID, HID, YBIT, 0, 3), (2 * HID, HID, YBIT, 0, 1))
FAR_Y = ((0, HID, XBIT | YBIT, 0, 1), (HID, HID // 2, XBIT | YBIT, 0, 3))
FAR_X = ((0, HID // 2, XBIT | YBIT, HID // 2, 3), (HID // 2, HID, XBIT | YBIT, 0, 2))


def main_kernel(tables, qu, iu, idx_ref, a_ref, *refs):
    b_refs, late_refs = refs[:len(tables)], refs[len(tables):len(tables) + 2]
    w_ref, bias_ref, inv_ref, z_ref, out_ref, a_v, c_v, b_v, l_v, o_v, sa, sb = refs[len(tables) + 2:]
    me = idx_ref[0]
    chip, core = me // 2, lax.rem(me, 2)
    lanes = lambda n: pl.ds(pl.multiple_of(n * LANES, LANES), LANES)
    first_copies = []
    for r in range(4):
        target = c_v if r == 0 else a_v.at[:, lanes(r - 1)]
        first_copies.append(pltpu.make_async_copy(a_ref.at[:, lanes(chip ^ r)], target, sa.at[r]))
    for n, ref in enumerate(late_refs):
        seqs = ref.shape[1]
        at = pl.ds(pl.multiple_of((core ^ n) * seqs, seqs), seqs)
        first_copies.append(pltpu.make_async_copy(ref, l_v.at[:, at, :], sa.at[4 + n]))
    width = b_refs[0].shape[1]
    groups = b_v.shape[0] // qu
    b_copies = [[] for _ in range(groups)]
    for ref, (core_bit, table) in zip(b_refs, tables):
        for first, rows, k, q, r in table:
            js = pl.ds(pl.multiple_of((me ^ k ^ core_bit) * width, width), width)
            for part in range(rows // qu):
                src = ref.at[pl.ds(first + part * qu, qu)]
                g = q // qu + part
                b_copies[g].append(pltpu.make_async_copy(src, b_v.at[pl.ds(g * qu, qu), js, lanes(r - 1)], sb.at[g, len(b_copies[g])]))
    for c in first_copies + [c for group in b_copies for c in group]:
        c.start()
    for c in first_copies:
        c.wait()

    def ready(g):
        for n in range(groups):
            @pl.when(g == n)
            def _(n=n):
                for c in b_copies[n]:
                    c.wait()

    outer_rows(a_v, b_v, o_v, qu, ready=ready, more=(c_v, l_v))

    def store(i, r):
        out_ref[i] = z_ref[i] + ((r + bias_ref[...]) * inv_ref[pl.ds(i, 1), :]).T

    weigh_rows(w_ref, o_v, iu, store)


def main_rows(me, a, b_parts, tables, late, w_t, bias, inv, z, qu=8, iu=8):
    rows, cols, _ = z.shape
    hid = a.shape[0] // rows
    pieces = sum(piece[1] for _, table in tables for piece in table) // hid
    whole = lambda v: pl.BlockSpec(v.shape, lambda s, i: (0,) * v.ndim)
    return pl.pallas_call(
        functools.partial(main_kernel, tables, qu, iu),
        grid_spec=pltpu.PrefetchScalarGridSpec(
            num_scalar_prefetch=1,
            grid=(1,),
            in_specs=[ANY] * (len(b_parts) + 3) + [whole(w_t), whole(bias), whole(inv), whole(z)],
            out_specs=whole(z),
            scratch_shapes=[
                pltpu.VMEM((rows * hid, 3 * LANES), BF16),
                pltpu.VMEM((rows * hid, LANES), BF16),
                pltpu.VMEM((hid, cols, 3 * LANES), BF16),
                pltpu.VMEM((hid, LANES, cols), BF16),
                pltpu.VMEM((rows, hid, hid, cols), BF16),
                pltpu.SemaphoreType.DMA((6,)),
                pltpu.SemaphoreType.DMA((hid // qu, pieces)),
            ],
        ),
        out_shape=jax.ShapeDtypeStruct(z.shape, F32),
        compiler_params=pltpu.CompilerParams(vmem_limit_bytes=48 << 20),
        cost_estimate=pl.CostEstimate(flops=12 << 30, bytes_accessed=20 << 20, transcendentals=0),
        name='main_outer',
    )(me, a, *b_parts, *late, w_t, bias, inv, z)


def combine_kernel(base_ref, inv_ref, lower_ref, upper_ref, *refs):
    step = pl.program_id(0)
    out_ref = refs[-1]

    def add(ref):
        for i in range(out_ref.shape[0]):
            total = ref[i].astype(F32)
            if len(refs) > 1:
                total = total + refs[0][i].astype(F32) + refs[1][...]
            row = step * out_ref.shape[0] + i
            out_ref[i] = base_ref[i] + (total * inv_ref[pl.ds(row, 1), :]).T

    @pl.when(step < pl.num_programs(0) // 2)
    def _():
        add(lower_ref)

    @pl.when(step >= pl.num_programs(0) // 2)
    def _():
        add(upper_ref)


def combine(base, inv, lower, upper, own=None, bias=None, block=16):
    rows, cols, chans = base.shape
    mid = rows // block // 2
    flat = lambda: pl.BlockSpec((block, cols, chans), lambda s: (s, 0, 0))
    extra, extra_specs = (), []
    if own is not None:
        extra = (own, bias)
        extra_specs = [pl.BlockSpec((block, chans, cols), lambda s: (s, 0, 0)), pl.BlockSpec((chans, cols), lambda s: (0, 0))]
    return pl.pallas_call(
        combine_kernel,
        grid=(2 * mid,),
        in_specs=[
            flat(),
            pl.BlockSpec((rows, cols), lambda s: (0, 0)),
            pl.BlockSpec((block, chans, cols), lambda s: (jnp.minimum(s, mid - 1), 0, 0)),
            pl.BlockSpec((block, chans, cols), lambda s: (jnp.maximum(s - mid, 0), 0, 0)),
        ] + extra_specs,
        out_specs=flat(),
        out_shape=jax.ShapeDtypeStruct(base.shape, F32),
        compiler_params=pltpu.CompilerParams(vmem_limit_bytes=24 << 20),
        cost_estimate=pl.CostEstimate(flops=1 << 24, bytes_accessed=15 << 20, transcendentals=0),
        name='combine',
    )(base, inv, lower, upper, *extra)


def assemble_kernel(ref, out_ref):
    width = ref.shape[2]
    for d in range(ref.shape[0]):
        out_ref[:, d * width:(d + 1) * width, :] = ref[d]


def assemble(value, block=8):
    srcs, seqs, width, chans = value.shape
    return pl.pallas_call(
        assemble_kernel,
        grid=(seqs // block,),
        in_specs=[pl.BlockSpec((srcs, block, width, chans), lambda s: (0, s, 0, 0))],
        out_specs=pl.BlockSpec((block, srcs * width, chans), lambda s: (s, 0, 0)),
        out_shape=jax.ShapeDtypeStruct((seqs, srcs * width, chans), value.dtype),
        cost_estimate=pl.CostEstimate(flops=1 << 24, bytes_accessed=16 << 20, transcendentals=0),
        name='assemble',
    )(value)


def layer_norm(value, gamma, beta):
    as_float = value.astype(F32)
    mean = jnp.mean(as_float, axis=-1, keepdims=True)
    centered = as_float - mean
    var = jnp.mean(centered * centered, axis=-1, keepdims=True)
    return (centered * lax.rsqrt(var + LN_EPS) * gamma.astype(F32) + beta.astype(F32)).astype(BF16)


def inverse_norms(mask, mask_rows):
    counts = jnp.einsum('si,sj->ij', mask_rows.astype(BF16), mask.astype(BF16), preferred_element_type=F32)
    return 1.0 / (NORM_EPS + counts)


def solution(mesh):
    size = mesh.shape['dap']
    value_spec = P('data', 'dap', None)
    mask_spec = P('data', None)
    row_spec = P(('data', 'dap'), None, None)

    def local_program(extra_block, extra_mask, main_block, main_mask, pair_rows, eg, eb, ewl, ebl, ewr, ebr, ewo, ebo, mg, mb, mwl, mbl, mwr, mbr, mwo, mbo):
        me = lax.axis_index('dap')
        chip = me // 2
        rows = extra_block.shape[1]
        hid = ewl.shape[1]

        seqs = extra_block.shape[0] // size
        cols = size * rows
        minor = extra_block.transpose(1, 2, 0)
        me1 = me.astype(jnp.int32)[None]
        turned = dict(zip(NEAR[:2], turn(me1, minor, NEAR[:2], size)))
        turned.update(zip(NEAR[2:], turn(me1, minor, NEAR[2:], size)))
        turned.update(zip(REST, turn(me1, minor, REST, size)))
        blocks = {0: turned[0]}
        for k in NEAR[:2]:
            blocks[k] = swap(turned[k], k, size)
        for k in NEAR[2:]:
            blocks[k] = swap(turned[k], k, size)
        blocks[1] = swap(turned[1], CORE, size)
        near, far = lax.optimization_barrier(([blocks[k] for k in NEAR], [turned[6], turned[7]]))
        blocks.update(zip(NEAR, near))
        for k, value in zip((6, 7), far):
            blocks[k] = swap(value, k, size)

        mask_rows_m = lax.dynamic_slice_in_dim(main_mask, me * rows, rows, axis=1)
        normed = layer_norm(main_block, mg, mb)
        mask_m = mask_rows_m.astype(F32).T

        wide = lambda v, n: jnp.broadcast_to(v.astype(F32)[:, None], (v.shape[0], n))
        mask_seq = lax.dynamic_slice_in_dim(extra_mask, me * seqs, seqs, axis=0).astype(F32).T
        w_both, bias = project_weights(ewl, ebl, ewr, ebr, seqs)
        gamma, beta = wide(eg, seqs), wide(eb, seqs)
        idx_a, idx_b = [(me ^ jnp.array(ks, jnp.int32)).astype(jnp.int32) for ks in (SET_A, SET_B)]
        a_m = jnp.einsum('sim,mp->ips', normed, mwl, preferred_element_type=F32) + mbl.astype(F32)[None, :, None]
        a_m = (a_m * mask_m[:, None, :]).astype(BF16).reshape(rows * hid, -1)
        b_m = jnp.einsum('sim,mq->qis', normed, mwr, preferred_element_type=F32) + mbr.astype(F32)[:, None, None]
        b_m = (b_m * mask_m[None]).astype(BF16)
        pick = lambda r: lax.dynamic_slice_in_dim(b_m, (chip ^ r) * LANES, LANES, axis=2)
        b_0, b_1, b_2, b_3 = [pick(r) for r in range(4)]
        b_to_x, b_to_y = jnp.concatenate([b_3, b_2, b_0]), jnp.concatenate([b_0, b_1, b_3])
        mask_rows_e = lax.dynamic_slice_in_dim(extra_mask, me * rows, rows, axis=1)
        inv_m = inverse_norms(main_mask, mask_rows_m)
        inv_e = inverse_norms(extra_mask, mask_rows_e)
        w_e, w_m = turn_weights(ewo, hid), turn_weights(mwo, hid)
        bias_e, bias_m = wide(ebo, cols), wide(mbo, cols)
        count = main_mask.shape[0] // size
        mask_late = lax.dynamic_slice_in_dim(main_mask, me * count, count, axis=0).astype(F32)

        a_a, a_a_give, b_a = project(idx_a, [blocks[k] for k in SET_A], mask_seq, gamma, beta, w_both, bias, hid)
        a_a_sib, b_a_sib = swap(a_a_give, CORE, size), swap(b_a, CORE, size)

        blocks[6], blocks[7], main_moved = lax.optimization_barrier((blocks[6], blocks[7], main_block))
        main_moved = lax.all_to_all(main_moved, 'dap', 0, 0, tiled=True).reshape(size, -1, rows, main_block.shape[2])
        b_x, b_y = swap(b_to_x, XBIT, size), swap(b_to_y, YBIT, size)
        b_dx, b_dy = swap(b_y[hid // 2:2 * hid], XBIT, size), swap(b_x[hid:2 * hid + hid // 2], YBIT, size)
        b_parts = [b_to_x, b_to_y, b_x, b_y]
        b_parts = b_parts + [swap(part, CORE, size) for part in b_parts]
        b_parts = b_parts + [b_dx, b_dy, swap(b_dx, CORE, size), swap(b_dy, CORE, size)]
        near_tables, far_tables = (OWN_X, OWN_Y, FROM_X, FROM_Y), (FAR_X, FAR_Y)
        tables = tuple((bit, t) for ts in (near_tables, far_tables) for bit in (0, CORE) for t in ts)
        late = main_late(main_moved, mask_late, mg, mb, mwr, mbr)
        late_sib = swap(late, CORE, size)

        a_b, a_b_give, b_b = project(idx_b, [blocks[k] for k in SET_B], mask_seq, gamma, beta, w_both, bias, hid)
        a_b_sib, b_b_sib = swap(a_b_give, CORE, size), swap(b_b, CORE, size)
        fx, fy, nx, ny, kx, ky, own = extra_parts(me1, (a_a, a_a_sib, a_b, a_b_sib), (b_a, b_a_sib, b_b, b_b_sib), w_e, cols)
        fx, fy = swap(fx, XBIT, size), swap(fy, YBIT, size)
        nx, ny = swap(nx, XBIT, size), swap(ny, YBIT, size)
        kx = (kx.astype(F32) + fy.astype(F32)).astype(BF16)
        ky = (ky.astype(F32) + fx.astype(F32)).astype(BF16)
        kx, ky = swap(kx, XBIT, size), swap(ky, YBIT, size)

        base = main_rows(me1, a_m, b_parts, tables, (late, late_sib), w_m, bias_m, inv_m, pair_rows)
        main_out = assemble(main_moved)
        extra_out = turn_out(me1, blocks, (0, 1, 2, 3), size)
        extra_out = turn_out(me1, blocks, (4, 5, 6, 7), size, extra_out).transpose(0, 2, 1)
        base = combine(base, inv_e, nx, ny, own, bias_e)
        pair_out = combine(base, inv_e, ky, kx)
        return pair_out, extra_out, main_out

    in_specs = (value_spec, mask_spec, value_spec, mask_spec, row_spec) + (P(),) * 16
    return jax.shard_map(local_program, mesh=mesh, in_specs=in_specs, out_specs=(row_spec, row_spec, row_spec), check_vma=False)
```
